64 devices in a mesh: rep: 8 (over x, y, core), dp: 8 (over z).
Axes of the slice: x: 2, y: 2, z: 8, core: 2. Of those that a mesh axis runs over, the one named last changes fastest.
The devices are a block of a 4x4x8 slice.
Arguments:
- g_w_gate: bfloat16 [64, 2, 512, 1408], P(('rep', 'dp')), parts along dimension 0
- g_w_up: bfloat16 [64, 2, 512, 1408], P(('rep', 'dp')), parts along dimension 0
- g_w_down: bfloat16 [64, 2, 1408, 512], P(('rep', 'dp')), parts along dimension 0
- w_gate: bfloat16 [2, 512, 1408], replicated
- w_up: bfloat16 [2, 512, 1408], replicated
- w_down: bfloat16 [2, 1408, 512], replicated
- m_w_gate: float32 [2, 512, 1408], P(None, 'dp')
- m_w_up: float32 [2, 512, 1408], P(None, 'dp')
- m_w_down: float32 [2, 1408, 512], P(None, 'dp')
- v_w_gate: float32 [2, 512, 1408], P(None, 'dp')
- v_w_up: float32 [2, 512, 1408], P(None, 'dp')
- v_w_down: float32 [2, 1408, 512], P(None, 'dp')
Outputs:
- output 1: bfloat16 [16, 512, 1408], P('rep'), parts along dimension 0
- output 2: bfloat16 [16, 512, 1408], P('rep'), parts along dimension 0
- output 3: bfloat16 [16, 1408, 512], P('rep'), parts along dimension 0
- output 4: float32 [16, 512, 1408], P('rep', 'dp'), parts along dimension 0
- output 5: float32 [16, 512, 1408], P('rep', 'dp'), parts along dimension 0
- output 6: float32 [16, 1408, 512], P('rep', 'dp'), parts along dimension 0
- output 7: float32 [16, 512, 1408], P('rep', 'dp'), parts along dimension 0
- output 8: float32 [16, 512, 1408], P('rep', 'dp'), parts along dimension 0
- output 9: float32 [16, 1408, 512], P('rep', 'dp'), parts along dimension 0
There are 8 independent parts. The reference program is written for one: setup_inputs(seed, part) draws one part's arguments, and reference() takes and returns one part's arrays. A program takes and returns all parts, laid end to end along the dimension named above; an argument that names none is the same for every part.
All inputs are finite; a program needn't handle non-finite values.
Results may differ from the reference program's by a relative error of at most 0.022.
Values are sent between devices in bfloat16 or wider.
A program may use at most 768 MiB of HBM per device.

```python
import jax
import jax.numpy as jnp
from jax import lax

DEVICES = 8
D = 512
FF = 1408
LAYERS = 2
NAMES = ("w_gate", "w_up", "w_down")
SHAPES = {"w_gate": (LAYERS, D, FF), "w_up": (LAYERS, D, FF), "w_down": (LAYERS, FF, D)}


def setup_inputs(seed: int = 0, part: int = 0) -> dict:
    kz, *keys = jax.random.split(jax.random.key(seed), 1 + 5 * len(NAMES))
    loud = 2.0 ** jax.random.uniform(kz, (), jnp.float32, -1.0, 1.0)
    drawn = {}
    for name, key, both in zip(NAMES, keys[:3], keys[3:6], strict=True):
        own = jax.random.normal(jax.random.fold_in(key, part), (DEVICES, *SHAPES[name]), jnp.float32)
        shared = jax.random.normal(jax.random.fold_in(both, part), SHAPES[name], jnp.float32)
        drawn["g_" + name] = (loud * (0.7 * shared / DEVICES + 0.7 * own * DEVICES**-0.5)).astype(jnp.bfloat16)
    for name, key in zip(NAMES, keys[6:9], strict=True):
        drawn[name] = (jax.random.normal(key, SHAPES[name], jnp.float32) * SHAPES[name][1] ** -0.5).astype(jnp.bfloat16)
    for name, key in zip(NAMES, keys[9:12], strict=True):
        drawn["m_" + name] = loud * 0.5 * jax.random.normal(key, SHAPES[name], jnp.float32)
    for name, key in zip(NAMES, keys[12:15], strict=True):
        drawn["v_" + name] = loud * loud * jax.random.uniform(key, SHAPES[name], jnp.float32, 0.5, 1.5)
    return drawn


def adamw(w, m, v, g):
    m = 0.9 * m + 0.1 * g
    v = 0.95 * v + 0.05 * g * g
    step = m * lax.rsqrt(v + 1e-8) + 0.1 * w
    return (w - 0.02 * step).astype(jnp.bfloat16), m, v


def reference(g_w_gate, g_w_up, g_w_down, w_gate, w_up, w_down, m_w_gate, m_w_up, m_w_down, v_w_gate, v_w_up, v_w_down):
    def total(terms):
        return lax.scan(lambda so_far, term: (so_far + term.astype(jnp.float32), None), jnp.zeros(terms.shape[1:], jnp.float32), terms)[0]

    gradients = [total(terms).astype(jnp.bfloat16).astype(jnp.float32) for terms in (g_w_gate, g_w_up, g_w_down)]
    new = [
        adamw(w.astype(jnp.float32), m, v, g)
        for w, m, v, g in zip((w_gate, w_up, w_down), (m_w_gate, m_w_up, m_w_down), (v_w_gate, v_w_up, v_w_down), gradients, strict=True)
    ]
    return tuple(one[which] for which in range(3) for one in new)
```

```python
import functools

import jax
import jax.numpy as jnp
from jax import lax
from jax.experimental import pallas as pl
from jax.experimental.pallas import tpu as pltpu
from jax.sharding import PartitionSpec as P

MESH = pl.DeviceIdType.MESH
ROWS = 16
VMEM = 54_000_000


def adamw(w, m, v, g):
    m = 0.9 * m + 0.1 * g
    v = 0.95 * v + 0.05 * g * g
    step = m * lax.rsqrt(v + 1e-8) + 0.1 * w
    return (w - 0.02 * step).astype(jnp.bfloat16), m, v


class Plan:
    def __init__(self, n, pieces):
        self.n, self.pieces = n, pieces
        far, near = n // 2, (n - 1) // 2
        self.hops = [(far, near) if p % 2 == 0 else (near, far) for p in range(pieces)]
        self.far = far

    def order(self, side, hops_left):
        live = [p for p in range(self.pieces) if self.hops[p][side] >= hops_left]
        if hops_left == self.far - 1:
            live.sort(key=lambda p: self.hops[p][side])
        return live

    def spread(self, side, hop):
        live = [p for p in range(self.pieces) if self.hops[p][side] >= hop]
        if hop == self.far - 1:
            live.sort(key=lambda p: -self.hops[p][side])
        return live


def kernel(plan, kinds, names, *refs):
    n, pieces = plan.n, plan.pieces
    weights = len(names)
    g, w, m, v = (refs[i * weights : (i + 1) * weights] for i in range(4))
    w_out, m_out, v_out = (refs[(4 + i) * weights : (5 + i) * weights] for i in range(3))
    rest = list(refs[7 * weights :])
    terms, inbox, own, m_in, v_in = (rest[i * len(kinds) : (i + 1) * len(kinds)] for i in range(5))
    load_sem, state_sem, send_sem, recv_sem, gather_send_sem, gather_recv_sem = rest[5 * len(kinds) :]

    me = lax.axis_index("dp")
    to = [lax.rem(me + 1, n), lax.rem(me + n - 1, n)]
    at = lambda away: lax.rem(me + (away + n), n)

    layers = w[0].shape[0]
    where = []
    for p in range(pieces):
        k, layer = p // layers, p % layers
        kind, first = names[k]
        where.append((k, layer, kind, first * layers + layer))

    def rows(p, owner):
        r = m[where[p][0]].shape[1]
        return pl.ds(pl.multiple_of(owner * r, r), r)

    def signed(side, hops):
        return hops if side == 0 else -hops

    def term(p, away):
        _, _, kind, place = where[p]
        return terms[kind].at[place, away % n]

    def slot(p, side, hops_left):
        _, _, kind, place = where[p]
        return inbox[kind].at[place, side * plan.far + hops_left - 1]

    def load(p, away):
        k, layer, _, _ = where[p]
        return pltpu.make_async_copy(g[k].at[0, layer, rows(p, at(away))], term(p, away), load_sem.at[p, away % n])

    def state_loads(k):
        kind, first = names[k]
        mine = pl.ds(first * layers, layers)
        block = rows(k * layers, me)
        return [
            pltpu.make_async_copy(w[k].at[:, block], own[kind].at[mine], state_sem.at[k, 0]),
            pltpu.make_async_copy(m[k], m_in[kind].at[mine], state_sem.at[k, 1]),
            pltpu.make_async_copy(v[k], v_in[kind].at[mine], state_sem.at[k, 2]),
        ]

    loads = {}
    first_wave = [(p, s, plan.hops[p][s]) for h in (plan.far, plan.far - 1) for p in range(pieces) for s in (0, 1) if plan.hops[p][s] == h]
    wanted = [(p, signed(s, h)) for p, s, h in first_wave]
    for h in range(plan.far - 1, 0, -1):
        wanted += [(p, signed(s, h)) for p in range(pieces) for s in (0, 1)]
    wanted += [(p, 0) for p in range(pieces)]
    for p, away in wanted:
        if (p, away % n) not in loads:
            loads[p, away % n] = load(p, away)
            loads[p, away % n].start()
    states = [state_loads(k) for k in range(weights)]
    for copies in states:
        for copy in copies:
            copy.start()

    barrier = pltpu.get_barrier_semaphore()
    for neighbour in to:
        pl.semaphore_signal(barrier, inc=1, device_id={"dp": neighbour}, device_id_type=MESH)
    pl.semaphore_wait(barrier, 2)

    def reduce_copy(p, side, hops_left):
        return pltpu.make_async_remote_copy(
            src_ref=term(p, signed(side, hops_left)),
            dst_ref=slot(p, side, hops_left),
            send_sem=send_sem.at[p, side, hops_left - 1],
            recv_sem=recv_sem.at[p, side, hops_left - 1],
            device_id={"dp": to[side]},
            device_id_type=MESH,
        )

    def by_rows(ref, body):
        lax.fori_loop(0, ref.shape[0] // ROWS, lambda i, _: body(pl.ds(pl.multiple_of(i * ROWS, ROWS), ROWS)), None)

    def add(into, other):
        def body(r):
            into[r, :] = (into[r, :].astype(jnp.float32) + other[r, :].astype(jnp.float32)).astype(jnp.bfloat16)

        by_rows(into, body)

    sent = []
    waited = set()

    def loaded(p, away):
        if (p, away % n) not in waited:
            waited.add((p, away % n))
            loads[p, away % n].wait()

    for h in range(plan.far, 0, -1):
        order = [plan.order(s, h) for s in (0, 1)]
        for i in range(max(map(len, order))):
            for s in (0, 1):
                if i >= len(order[s]):
                    continue
                p = order[s][i]
                loaded(p, signed(s, h))
                if plan.hops[p][s] > h:
                    reduce_copy(p, s, h + 1).wait_recv()
                    add(term(p, signed(s, h)), slot(p, s, h + 1))
                copy = reduce_copy(p, s, h)
                copy.start()
                sent.append(copy)

    def gather_copy(p, side, hop, back):
        k, layer, _, _ = where[p]
        block = w_out[k].at[layer, rows(p, at(-signed(side, hop - back)))]
        return pltpu.make_async_remote_copy(
            src_ref=block,
            dst_ref=block,
            send_sem=gather_send_sem.at[p, side, hop - 1],
            recv_sem=gather_recv_sem.at[p, side, hop - 1],
            device_id={"dp": to[side]},
            device_id_type=MESH,
        )

    def step(p):
        k, layer, kind, place = where[p]
        first_row = me * m[k].shape[1]

        def body(r):
            total = term(p, 0)[r, :].astype(jnp.float32)
            for s in (0, 1):
                total += slot(p, s, 1)[r, :].astype(jnp.float32)
            total = total.astype(jnp.bfloat16).astype(jnp.float32)
            new = adamw(own[kind].at[place][r, :].astype(jnp.float32), m_in[kind].at[place][r, :], v_in[kind].at[place][r, :], total)
            w_out[k].at[layer][pl.ds(pl.multiple_of(first_row + r.start, ROWS), ROWS), :] = new[0]
            m_out[k].at[layer][r, :] = new[1]
            v_out[k].at[layer][r, :] = new[2]

        by_rows(term(p, 0), body)

    for p in range(pieces):
        k, layer, _, _ = where[p]
        if layer == 0:
            for copy in states[k]:
                copy.wait()
        loaded(p, 0)
        for s in (0, 1):
            reduce_copy(p, s, 1).wait_recv()
        step(p)
        for s in (0, 1):
            copy = gather_copy(p, s, 1, 1)
            copy.start()
            sent.append(copy)

    for hop in range(2, plan.far + 1):
        order = [plan.spread(s, hop) for s in (0, 1)]
        for i in range(max(map(len, order))):
            for s in (0, 1):
                if i < len(order[s]):
                    p = order[s][i]
                    gather_copy(p, s, hop - 1, 0).wait_recv()
                    copy = gather_copy(p, s, hop, 1)
                    copy.start()
                    sent.append(copy)
    for p in range(pieces):
        for s in (0, 1):
            gather_copy(p, s, plan.hops[p][s], 0).wait_recv()
    for copy in sent:
        copy.wait_send()


def solution(mesh):
    n = mesh.shape["dp"]

    def step(*arrays):
        g, w, m, v = (arrays[i : i + 3] for i in (0, 3, 6, 9))
        layers = w[0].shape[0]
        plan = Plan(n, layers * len(w))
        kinds, names = [], []
        for one in m:
            if one.shape[1:] not in kinds:
                kinds.append(one.shape[1:])
            kind = kinds.index(one.shape[1:])
            names.append((kind, sum(1 for other, _ in names if other == kind)))
        count = [layers * sum(1 for kind, _ in names if kind == i) for i in range(len(kinds))]
        places = list(zip(count, kinds, strict=True))
        hbm, vmem = pl.BlockSpec(memory_space=pltpu.HBM), pl.BlockSpec(memory_space=pltpu.VMEM)
        pieces, far = plan.pieces, plan.far
        dma = pltpu.SemaphoreType.DMA
        out = pl.pallas_call(
            functools.partial(kernel, plan, kinds, names),
            out_shape=[pltpu.VMEM(one.shape, one.dtype) for one in (*w, *m, *v)],
            in_specs=[hbm] * len(arrays),
            out_specs=[vmem] * 9,
            scratch_shapes=[
                *(pltpu.VMEM((c, n, *shape), jnp.bfloat16) for c, shape in places),
                *(pltpu.VMEM((c, 2 * far, *shape), jnp.bfloat16) for c, shape in places),
                *(pltpu.VMEM((c, *shape), jnp.bfloat16) for c, shape in places),
                *(pltpu.VMEM((c, *shape), jnp.float32) for c, shape in places),
                *(pltpu.VMEM((c, *shape), jnp.float32) for c, shape in places),
                dma((pieces, n)),
                dma((len(w), 3)),
                dma((pieces, 2, far)),
                dma((pieces, 2, far)),
                dma((pieces, 2, far)),
                dma((pieces, 2, far)),
            ],
            compiler_params=pltpu.CompilerParams(collective_id=0, has_side_effects=True, vmem_limit_bytes=VMEM),
        )(*arrays)
        return tuple(out)

    all_of, cut = P(None, None, None), P(None, "dp", None)
    return jax.shard_map(
        step,
        mesh=mesh,
        in_specs=(P(("rep", "dp"), None, None, None),) * 3 + (all_of,) * 3 + (cut,) * 6,
        out_specs=(P("rep", None, None),) * 3 + (P("rep", "dp", None),) * 6,
        check_vma=False,
    )
```

```python
import functools

import jax
import jax.numpy as jnp
from jax import lax
from jax.experimental import pallas as pl
from jax.experimental.pallas import tpu as pltpu
from jax.sharding import PartitionSpec as P

MESH = pl.DeviceIdType.MESH
ROWS = 16
VMEM = 54_000_000


def adamw(w, m, v, g):
    m = 0.9 * m + 0.1 * g
    v = 0.95 * v + 0.05 * g * g
    step = m * lax.rsqrt(v + 1e-8) + 0.1 * w
    return (w - 0.02 * step).astype(jnp.bfloat16), m, v


class Plan:
    def __init__(self, n, pieces):
        self.n, self.pieces = n, pieces
        far, near = n // 2, (n - 1) // 2
        self.hops = [(far, near) if p % 2 == 0 else (near, far) for p in range(pieces)]
        self.far = far

    def starts(self, side, hops_left):
        return [p for p in range(self.pieces) if self.hops[p][side] == hops_left]

    def order(self, side, hops_left):
        return [p for p in range(self.pieces) if self.hops[p][side] > hops_left]

    def spread(self, side, hop):
        live = [p for p in range(self.pieces) if self.hops[p][side] >= hop]
        if hop == self.far - 1:
            live.sort(key=lambda p: -self.hops[p][side])
        return live


def kernel(plan, kinds, names, *refs):
    n, pieces = plan.n, plan.pieces
    weights = len(names)
    g, w, m, v = (refs[i * weights : (i + 1) * weights] for i in range(4))
    w_out, m_out, v_out = (refs[(4 + i) * weights : (5 + i) * weights] for i in range(3))
    rest = list(refs[7 * weights :])
    terms, inbox, own, m_in, v_in = (rest[i * len(kinds) : (i + 1) * len(kinds)] for i in range(5))
    load_sem, state_sem, send_sem, recv_sem, gather_send_sem, gather_recv_sem = rest[5 * len(kinds) :]

    me = lax.axis_index("dp")
    to = [lax.rem(me + 1, n), lax.rem(me + n - 1, n)]
    at = lambda away: lax.rem(me + (away + n), n)

    layers = w[0].shape[0]
    where = []
    for p in range(pieces):
        k, layer = p // layers, p % layers
        kind, first = names[k]
        where.append((k, layer, kind, first * layers + layer))

    def rows(p, owner):
        r = m[where[p][0]].shape[1]
        return pl.ds(pl.multiple_of(owner * r, r), r)

    def signed(side, hops):
        return hops if side == 0 else -hops

    def term(p, away):
        _, _, kind, place = where[p]
        return terms[kind].at[place, away % n]

    def slot(p, side, hops_left):
        _, _, kind, place = where[p]
        return inbox[kind].at[place, side * plan.far + hops_left - 1]

    def load(p, away):
        k, layer, _, _ = where[p]
        return pltpu.make_async_copy(g[k].at[0, layer, rows(p, at(away))], term(p, away), load_sem.at[p, away % n])

    def state_loads(k):
        kind, first = names[k]
        mine = pl.ds(first * layers, layers)
        block = rows(k * layers, me)
        return [
            pltpu.make_async_copy(w[k].at[:, block], own[kind].at[mine], state_sem.at[k, 0]),
            pltpu.make_async_copy(m[k], m_in[kind].at[mine], state_sem.at[k, 1]),
            pltpu.make_async_copy(v[k], v_in[kind].at[mine], state_sem.at[k, 2]),
        ]

    barrier = pltpu.get_barrier_semaphore()
    for neighbour in to:
        pl.semaphore_signal(barrier, inc=1, device_id={"dp": neighbour}, device_id_type=MESH)
    pl.semaphore_wait(barrier, 2)

    def reduce_copy(p, side, hops_left):
        k, layer, _, _ = where[p]
        away = signed(side, hops_left)
        first = plan.hops[p][side] == hops_left
        return pltpu.make_async_remote_copy(
            src_ref=g[k].at[0, layer, rows(p, at(away))] if first else term(p, away),
            dst_ref=slot(p, side, hops_left),
            send_sem=send_sem.at[p, side, hops_left - 1],
            recv_sem=recv_sem.at[p, side, hops_left - 1],
            device_id={"dp": to[side]},
            device_id_type=MESH,
        )

    def by_rows(ref, body):
        lax.fori_loop(0, ref.shape[0] // ROWS, lambda i, _: body(pl.ds(pl.multiple_of(i * ROWS, ROWS), ROWS)), None)

    def add(into, other):
        def body(r):
            into[r, :] = (into[r, :].astype(jnp.float32) + other[r, :].astype(jnp.float32)).astype(jnp.bfloat16)

        by_rows(into, body)

    sent, loads = [], {}
    for h in range(plan.far, 0, -1):
        for order in zip(*(plan.starts(s, h) for s in (0, 1)), strict=True):
            for s, p in enumerate(order):
                sent.append(reduce_copy(p, s, h))
                sent[-1].start()
    for h in range(plan.far - 1, -1, -1):
        for p in range(pieces):
            for away in sorted({h, -h}):
                if h == 0 or plan.hops[p][away < 0] > h:
                    loads[p, away] = load(p, away)
                    loads[p, away].start()
    states = [state_loads(k) for k in range(weights)]
    for copies in states:
        for copy in copies:
            copy.start()

    for h in range(plan.far - 1, 0, -1):
        for order in zip(*(plan.order(s, h) for s in (0, 1)), strict=True):
            for s, p in enumerate(order):
                away = signed(s, h)
                loads[p, away].wait()
                reduce_copy(p, s, h + 1).wait_recv()
                add(term(p, away), slot(p, s, h + 1))
                sent.append(reduce_copy(p, s, h))
                sent[-1].start()

    def gather_copy(p, side, hop, back):
        k, layer, _, _ = where[p]
        block = w_out[k].at[layer, rows(p, at(-signed(side, hop - back)))]
        return pltpu.make_async_remote_copy(
            src_ref=block,
            dst_ref=block,
            send_sem=gather_send_sem.at[p, side, hop - 1],
            recv_sem=gather_recv_sem.at[p, side, hop - 1],
            device_id={"dp": to[side]},
            device_id_type=MESH,
        )

    def step(p):
        k, layer, kind, place = where[p]
        first_row = me * m[k].shape[1]

        def body(r):
            total = term(p, 0)[r, :].astype(jnp.float32)
            for s in (0, 1):
                total += slot(p, s, 1)[r, :].astype(jnp.float32)
            total = total.astype(jnp.bfloat16).astype(jnp.float32)
            new = adamw(own[kind].at[place][r, :].astype(jnp.float32), m_in[kind].at[place][r, :], v_in[kind].at[place][r, :], total)
            w_out[k].at[layer][pl.ds(pl.multiple_of(first_row + r.start, ROWS), ROWS), :] = new[0]
            m_out[k].at[layer][r, :] = new[1]
            v_out[k].at[layer][r, :] = new[2]

        by_rows(term(p, 0), body)

    for p in range(pieces):
        k, layer, _, _ = where[p]
        if layer == 0:
            for copy in states[k]:
                copy.wait()
        loads[p, 0].wait()
        for s in (0, 1):
            reduce_copy(p, s, 1).wait_recv()
        step(p)
        for s in (0, 1):
            copy = gather_copy(p, s, 1, 1)
            copy.start()
            sent.append(copy)

    for hop in range(2, plan.far + 1):
        order = [plan.spread(s, hop) for s in (0, 1)]
        for i in range(max(map(len, order))):
            for s in (0, 1):
                if i < len(order[s]):
                    p = order[s][i]
                    gather_copy(p, s, hop - 1, 0).wait_recv()
                    copy = gather_copy(p, s, hop, 1)
                    copy.start()
                    sent.append(copy)
    for p in range(pieces):
        for s in (0, 1):
            gather_copy(p, s, plan.hops[p][s], 0).wait_recv()
    for copy in sent:
        copy.wait_send()


def put_kernel(count, *refs):
    sources, results, sem = refs[:count], refs[count:-1], refs[-1]
    copies = [pltpu.make_async_copy(a, b, sem.at[i]) for i, (a, b) in enumerate(zip(sources, results, strict=True))]
    for copy in copies:
        copy.start()
    for copy in copies:
        copy.wait()


def put(arrays):
    return pl.pallas_call(
        functools.partial(put_kernel, len(arrays)),
        out_shape=[pltpu.HBM(one.shape, one.dtype) for one in arrays],
        in_specs=[pl.BlockSpec(memory_space=pltpu.VMEM)] * len(arrays),
        out_specs=[pl.BlockSpec(memory_space=pltpu.HBM)] * len(arrays),
        scratch_shapes=[pltpu.SemaphoreType.DMA((len(arrays),))],
        compiler_params=pltpu.CompilerParams(vmem_limit_bytes=1 << 20),
    )(*arrays)


def solution(mesh):
    n = mesh.shape["dp"]

    def step(*arrays):
        g, w, m, v = (arrays[i : i + 3] for i in (0, 3, 6, 9))
        layers = w[0].shape[0]
        plan = Plan(n, layers * len(w))
        kinds, names = [], []
        for one in m:
            if one.shape[1:] not in kinds:
                kinds.append(one.shape[1:])
            kind = kinds.index(one.shape[1:])
            names.append((kind, sum(1 for other, _ in names if other == kind)))
        count = [layers * sum(1 for kind, _ in names if kind == i) for i in range(len(kinds))]
        places = list(zip(count, kinds, strict=True))
        hbm, vmem = pl.BlockSpec(memory_space=pltpu.HBM), pl.BlockSpec(memory_space=pltpu.VMEM)
        pieces, far = plan.pieces, plan.far
        dma = pltpu.SemaphoreType.DMA
        out = pl.pallas_call(
            functools.partial(kernel, plan, kinds, names),
            out_shape=[pltpu.VMEM(one.shape, one.dtype) for one in (*w, *m, *v)],
            in_specs=[hbm] * len(arrays),
            out_specs=[vmem] * 9,
            scratch_shapes=[
                *(pltpu.VMEM((c, n, *shape), jnp.bfloat16) for c, shape in places),
                *(pltpu.VMEM((c, 2 * far, *shape), jnp.bfloat16) for c, shape in places),
                *(pltpu.VMEM((c, *shape), jnp.bfloat16) for c, shape in places),
                *(pltpu.VMEM((c, *shape), jnp.float32) for c, shape in places),
                *(pltpu.VMEM((c, *shape), jnp.float32) for c, shape in places),
                dma((pieces, n)),
                dma((len(w), 3)),
                dma((pieces, 2, far)),
                dma((pieces, 2, far)),
                dma((pieces, 2, far)),
                dma((pieces, 2, far)),
            ],
            compiler_params=pltpu.CompilerParams(collective_id=0, has_side_effects=True, vmem_limit_bytes=VMEM),
        )(*arrays)
        return tuple(put(out))

    all_of, cut = P(None, None, None), P(None, "dp", None)
    return jax.shard_map(
        step,
        mesh=mesh,
        in_specs=(P(("rep", "dp"), None, None, None),) * 3 + (all_of,) * 3 + (cut,) * 6,
        out_specs=(P("rep", None, None),) * 3 + (P("rep", "dp", None),) * 6,
        check_vma=False,
    )
```

```python
import functools

import jax
import jax.numpy as jnp
from jax import lax
from jax.experimental import pallas as pl
from jax.experimental.pallas import tpu as pltpu
from jax.sharding import PartitionSpec as P

MESH = pl.DeviceIdType.MESH
DMA = pltpu.SemaphoreType.DMA
HBM, VMEM = pl.BlockSpec(memory_space=pltpu.HBM), pl.BlockSpec(memory_space=pltpu.VMEM)
ROWS = 16
GRANT_EARLY, GRANT_LATE = 57_000_000, 61_500_000


def adamw(w, m, v, g):
    m = 0.9 * m + 0.1 * g
    v = 0.95 * v + 0.05 * g * g
    step = m * lax.rsqrt(v + 1e-8) + 0.1 * w
    return (w - 0.02 * step).astype(jnp.bfloat16), m, v


def by_rows(count, body):
    lax.fori_loop(0, count // ROWS, lambda i, _: body(pl.multiple_of(i * ROWS, ROWS)), None)


def side_of(away):
    return 0 if away > 0 else 1


class Ring:
    def __init__(self, n, me, g, w, m, v, results, buffers, sems):
        self.n, self.me, self.g, self.w, self.m, self.v = n, me, g, w, m, v
        self.w_out, self.m_out, self.v_out = results
        self.terms, self.inbox, self.total, self.own, self.m_in, self.v_in = buffers
        self.load_sem, self.state_sem, self.send_sem, self.recv_sem, self.gather_send_sem, self.gather_recv_sem = sems
        self.to = [lax.rem(me + 1, n), lax.rem(me + n - 1, n)]
        self.layers = g[0].shape[1]
        self.pieces = len(g) * self.layers
        self.rows = g[0].shape[2] // n
        self.far = n // 2
        near = (n - 1) // 2
        self.hops = [(self.far, near) if p % 2 == 0 else (near, self.far) for p in range(self.pieces)]

    @staticmethod
    def buffers(n, pieces, shape, state):
        far = n // 2
        data = [pltpu.VMEM((pieces, n, *shape), jnp.bfloat16), pltpu.VMEM((pieces, 2, far, *shape), jnp.bfloat16)]
        if state:
            data += [pltpu.VMEM((pieces, *shape), t) for t in (jnp.bfloat16, jnp.bfloat16, jnp.float32, jnp.float32)]
        return data

    @staticmethod
    def sems(n, pieces, weights):
        far = n // 2
        return [DMA((pieces, n)), DMA((weights, 3)), *(DMA((pieces, 2, far)) for _ in range(4))]

    def at(self, away):
        return lax.rem(self.me + (away + self.n), self.n)

    def block(self, owner):
        return pl.ds(pl.multiple_of(owner * self.rows, self.rows), self.rows)

    def mine(self, p, away):
        return self.g[p // self.layers].at[0, p % self.layers, self.block(self.at(away))]

    def load(self, p, away):
        return pltpu.make_async_copy(self.mine(p, away), self.terms.at[p, away % self.n], self.load_sem.at[p, away % self.n])

    def remote(self, side, source, target, send_sem, recv_sem):
        return pltpu.make_async_remote_copy(
            src_ref=source, dst_ref=target, send_sem=send_sem, recv_sem=recv_sem, device_id={"dp": self.to[side]}, device_id_type=MESH
        )

    def sum_copy(self, p, side, left):
        away = left if side == 0 else -left
        source = self.mine(p, away) if self.hops[p][side] == left else self.terms.at[p, away % self.n]
        at = (p, side, left - 1)
        return self.remote(side, source, self.inbox.at[at], self.send_sem.at[at], self.recv_sem.at[at])

    def gather_copy(self, p, side, hop, back):
        away = hop - back
        block = self.w_out[p // self.layers].at[p % self.layers, self.block(self.at(-away if side == 0 else away))]
        at = (p, side, hop - 1)
        return self.remote(side, block, block, self.gather_send_sem.at[at], self.gather_recv_sem.at[at])

    def live(self, side, hops):
        return [p for p in range(self.pieces) if self.hops[p][side] >= hops]

    def first_terms(self):
        for left in range(self.far, 0, -1):
            for order in zip(*([p for p in range(self.pieces) if self.hops[p][s] == left] for s in (0, 1)), strict=True):
                for s, p in enumerate(order):
                    self.sum_copy(p, s, left).start()

    def loaded(self):
        return [
            (p, away)
            for left in range(self.far - 1, -1, -1)
            for p in range(self.pieces)
            for away in sorted({left, -left})
            if left == 0 or self.hops[p][side_of(away)] > left
        ]

    def load_terms(self):
        for p, away in self.loaded():
            self.load(p, away).start()

    def states(self, k):
        mine, block = pl.ds(k * self.layers, self.layers), self.block(self.me)
        return [
            pltpu.make_async_copy(self.w[k].at[:, block], self.own.at[mine], self.state_sem.at[k, 0]),
            pltpu.make_async_copy(self.m[k], self.m_in.at[mine], self.state_sem.at[k, 1]),
            pltpu.make_async_copy(self.v[k], self.v_in.at[mine], self.state_sem.at[k, 2]),
        ]

    def load_states(self):
        for k in range(len(self.g)):
            for copy in self.states(k):
                copy.start()

    def pass_on(self):
        for left in range(self.far - 1, 0, -1):
            for order in zip(*(self.live(s, left + 1) for s in (0, 1)), strict=True):
                for s, p in enumerate(order):
                    away = left if s == 0 else -left
                    self.load(p, away).wait()
                    self.sum_copy(p, s, left + 1).wait_recv()
                    here, came = self.terms.at[p, away % self.n], self.inbox.at[p, s, left]

                    def add(r, here=here, came=came):
                        r = pl.ds(r, ROWS)
                        here[r, :] = (here[r, :].astype(jnp.float32) + came[r, :].astype(jnp.float32)).astype(jnp.bfloat16)

                    by_rows(self.rows, add)
                    self.sum_copy(p, s, left).start()

    def finish_sum(self, p):
        self.load(p, 0).wait()
        for s in (0, 1):
            self.sum_copy(p, s, 1).wait_recv()

        def add(r):
            r = pl.ds(r, ROWS)
            parts = [ref[r, :].astype(jnp.float32) for ref in (self.terms.at[p, 0], self.inbox.at[p, 0, 0], self.inbox.at[p, 1, 0])]
            self.total.at[p][r, :] = (parts[0] + parts[1] + parts[2]).astype(jnp.bfloat16)

        by_rows(self.rows, add)

    def sums_sent(self):
        for p in range(self.pieces):
            for s in (0, 1):
                for left in range(1, self.hops[p][s] + 1):
                    self.sum_copy(p, s, left).wait_send()

    def step(self, p):
        k, layer = p // self.layers, p % self.layers
        if layer == 0:
            for copy in self.states(k):
                copy.wait()

        def take(r):
            rows = pl.ds(r, ROWS)
            w, m, v, g = (ref.at[p][rows, :] for ref in (self.own, self.m_in, self.v_in, self.total))
            new = adamw(w.astype(jnp.float32), m, v, g.astype(jnp.float32))
            self.w_out[k].at[layer][pl.ds(pl.multiple_of(self.me * self.rows + r, ROWS), ROWS), :] = new[0]
            self.m_out[k].at[layer][rows, :] = new[1]
            self.v_out[k].at[layer][rows, :] = new[2]

        by_rows(self.rows, take)
        for s in (0, 1):
            self.gather_copy(p, s, 1, 1).start()

    def gather(self):
        for hop in range(2, self.far + 1):
            order = [self.live(s, hop) for s in (0, 1)]
            for s in (0, 1):
                if hop == self.far - 1:
                    order[s].sort(key=lambda p, s=s: -self.hops[p][s])
            for pair in zip(*order, strict=True):
                for s, p in enumerate(pair):
                    self.gather_copy(p, s, hop - 1, 0).wait_recv()
                    self.gather_copy(p, s, hop, 1).start()
        for p in range(self.pieces):
            for s in (0, 1):
                self.gather_copy(p, s, self.hops[p][s], 0).wait_recv()
                for hop in range(1, self.hops[p][s] + 1):
                    self.gather_copy(p, s, hop, 1).wait_send()

    def greet(self):
        barrier = pltpu.get_barrier_semaphore()
        for neighbour in self.to:
            pl.semaphore_signal(barrier, inc=1, device_id={"dp": neighbour}, device_id_type=MESH)
        pl.semaphore_wait(barrier, 2)


def odd():
    return lax.rem(lax.axis_index("rep"), 2) == 1


def even():
    return lax.rem(lax.axis_index("rep"), 2) == 0


def early_kernel(n, count, *refs):
    refs = list(refs)
    take = lambda c: [refs.pop(0) for _ in range(c)]
    e, l = count
    g, w, m, v, late_g = take(e), take(e), take(e), take(e), take(l)
    results, late_total = [take(e) for _ in range(3)], refs.pop(0)
    me = lax.axis_index("dp")
    ring = Ring(n, me, g, w, m, v, results, take(6), take(6))
    terms, inbox = take(2)
    late = Ring(n, me, late_g, None, None, None, (None,) * 3, (terms, inbox, late_total, None, None, None), take(6))

    ring.greet()

    @pl.when(odd())
    def _():
        late.first_terms()

    ring.first_terms()

    @pl.when(odd())
    def _():
        late.load_terms()

    ring.load_terms()
    ring.load_states()

    @pl.when(odd())
    def _():
        late.pass_on()
        for p in range(late.pieces):
            late.finish_sum(p)
        late.sums_sent()

    ring.pass_on()
    for p in range(ring.pieces):
        ring.finish_sum(p)
        ring.step(p)
    ring.gather()
    ring.sums_sent()


def late_kernel(n, count, *refs):
    refs = list(refs)
    take = lambda c: [refs.pop(0) for _ in range(c)]
    g, w, m, v, total = take(count), take(count), take(count), take(count), refs.pop(0)
    results = [take(count) for _ in range(3)]
    ring = Ring(n, lax.axis_index("dp"), g, w, m, v, results, take(6), take(6))
    total_sem = refs.pop(0)
    ring.greet()

    @pl.when(even())
    def _():
        ring.first_terms()
        ring.load_terms()

    ring.load_states()

    @pl.when(odd())
    def _():
        copy = pltpu.make_async_copy(total, ring.total, total_sem)
        copy.start()
        copy.wait()

    @pl.when(even())
    def _():
        ring.pass_on()
        for p in range(ring.pieces):
            ring.finish_sum(p)
        ring.sums_sent()

    for p in range(ring.pieces):
        ring.step(p)
    ring.gather()


def put_kernel(count, *refs):
    sources, results, sem = refs[:count], refs[count:-1], refs[-1]
    copies = [pltpu.make_async_copy(a, b, sem.at[i]) for i, (a, b) in enumerate(zip(sources, results, strict=True))]
    for copy in copies:
        copy.start()
    for copy in copies:
        copy.wait()


def put(arrays):
    count = len(arrays)
    return pl.pallas_call(
        functools.partial(put_kernel, count),
        out_shape=[pltpu.HBM(one.shape, one.dtype) for one in arrays],
        in_specs=[VMEM] * count,
        out_specs=[HBM] * count,
        scratch_shapes=[DMA((count,))],
        compiler_params=pltpu.CompilerParams(vmem_limit_bytes=1 << 20),
    )(*arrays)


def solution(mesh):
    n = mesh.shape["dp"]

    def step(*arrays):
        g, w, m, v = (arrays[i : i + 3] for i in (0, 3, 6, 9))
        early, late = slice(0, 2), slice(2, 3)
        e, l = len(g[early]), len(g[late])
        layers = w[0].shape[0]
        vmem = lambda several: [pltpu.VMEM(one.shape, one.dtype) for one in several]
        early_shape, late_shape = m[early][0].shape[1:], m[late][0].shape[1:]

        *first, total = pl.pallas_call(
            functools.partial(early_kernel, n, (e, l)),
            out_shape=[*vmem((*w[early], *m[early], *v[early])), pltpu.VMEM((l * layers, *late_shape), jnp.bfloat16)],
            in_specs=[HBM] * (4 * e + l),
            out_specs=[VMEM] * (3 * e + 1),
            scratch_shapes=[
                *Ring.buffers(n, e * layers, early_shape, True),
                *Ring.sems(n, e * layers, e),
                *Ring.buffers(n, l * layers, late_shape, False),
                *Ring.sems(n, l * layers, l),
            ],
            compiler_params=pltpu.CompilerParams(collective_id=0, has_side_effects=True, vmem_limit_bytes=GRANT_EARLY),
        )(*g[early], *w[early], *m[early], *v[early], *g[late])
        *first, total = put([*first, total])
        second = pl.pallas_call(
            functools.partial(late_kernel, n, l),
            out_shape=vmem((*w[late], *m[late], *v[late])),
            in_specs=[HBM] * (4 * l + 1),
            out_specs=[VMEM] * (3 * l),
            scratch_shapes=[*Ring.buffers(n, l * layers, late_shape, True), *Ring.sems(n, l * layers, l), DMA],
            compiler_params=pltpu.CompilerParams(collective_id=1, has_side_effects=True, vmem_limit_bytes=GRANT_LATE),
        )(*g[late], *w[late], *m[late], *v[late], total)
        second = put(second)
        return tuple(one for i in range(3) for one in (*first[i * e : (i + 1) * e], *second[i * l : (i + 1) * l]))

    all_of, cut = P(None, None, None), P(None, "dp", None)
    return jax.shard_map(
        step,
        mesh=mesh,
        in_specs=(P(("rep", "dp"), None, None, None),) * 3 + (all_of,) * 3 + (cut,) * 6,
        out_specs=(P("rep", None, None),) * 3 + (P("rep", "dp", None),) * 6,
        check_vma=False,
    )
```

```python
import functools

import jax
import jax.numpy as jnp
from jax import lax
from jax.experimental import pallas as pl
from jax.experimental.pallas import tpu as pltpu
from jax.sharding import PartitionSpec as P

MESH = pl.DeviceIdType.MESH
DMA = pltpu.SemaphoreType.DMA
HBM, VMEM = pl.BlockSpec(memory_space=pltpu.HBM), pl.BlockSpec(memory_space=pltpu.VMEM)
ROWS = 16
EARLY_PIECES, LATE_PIECES = 2, 4
GRANT_EARLY, GRANT_LATE = 57_000_000, 61_500_000


def adamw(w, m, v, g):
    m = 0.9 * m + 0.1 * g
    v = 0.95 * v + 0.05 * g * g
    step = m * lax.rsqrt(v + 1e-8) + 0.1 * w
    return (w - 0.02 * step).astype(jnp.bfloat16), m, v


def by_rows(count, body):
    lax.fori_loop(0, count // ROWS, lambda i, _: body(pl.multiple_of(i * ROWS, ROWS)), None)


def side_of(away):
    return 0 if away > 0 else 1


class Ring:
    def __init__(self, n, me, pieces, g, w, m, v, results, buffers, sems):
        self.n, self.me, self.g, self.w, self.m, self.v = n, me, g, w, m, v
        self.w_out, self.m_out, self.v_out = results
        self.terms, self.inbox, self.total, self.own, self.m_in, self.v_in = buffers
        self.load_sem, self.state_sem, self.send_sem, self.recv_sem, self.gather_send_sem, self.gather_recv_sem = sems
        self.to = [lax.rem(me + 1, n), lax.rem(me + n - 1, n)]
        self.layers = g[0].shape[1]
        self.block_rows = g[0].shape[2] // n
        self.parts = self.cut(len(g), self.layers, self.block_rows, pieces)
        self.pieces = len(self.parts)
        self.far = n // 2
        near = (n - 1) // 2
        self.hops = [(self.far, near) if turn == 0 else (near, self.far) for *_, turn in self.parts]

    @staticmethod
    def cut(weights, layers, rows, pieces):
        size = -(-rows // (pieces * ROWS)) * ROWS
        starts = range(0, rows, size)
        return [(k, layer, r, min(size, rows - r), (i + layer) % 2) for k in range(weights) for layer in range(layers) for i, r in enumerate(starts)]

    @classmethod
    def buffers(cls, n, pieces, weights, layers, shape, state):
        far = n // 2
        parts = cls.cut(weights, layers, shape[0], pieces)
        pieces, whole = len(parts), (weights * layers, *shape)
        shape = (parts[0][3], shape[1])
        data = [pltpu.VMEM((pieces, n, *shape), jnp.bfloat16), pltpu.VMEM((pieces, 2, far, *shape), jnp.bfloat16)]
        if state:
            data += [pltpu.VMEM(whole, t) for t in (jnp.bfloat16, jnp.bfloat16, jnp.float32, jnp.float32)]
        return data

    @classmethod
    def sems(cls, n, pieces, weights, layers, shape):
        far = n // 2
        pieces = len(cls.cut(weights, layers, shape[0], pieces))
        return [DMA((pieces, n)), DMA((weights, 3)), *(DMA((pieces, 2, far)) for _ in range(4))]

    def at(self, away):
        return lax.rem(self.me + (away + self.n), self.n)

    def block(self, owner):
        return pl.ds(pl.multiple_of(owner * self.block_rows, self.block_rows), self.block_rows)

    def rows(self, p, owner):
        _, _, first, count, _ = self.parts[p]
        return pl.ds(pl.multiple_of(owner * self.block_rows + first, ROWS), count)

    def term(self, p, away):
        return self.terms.at[p, away % self.n, pl.ds(0, self.parts[p][3])]

    def came(self, p, side, left):
        return self.inbox.at[p, side, left - 1, pl.ds(0, self.parts[p][3])]

    def mine(self, p, away):
        k, layer, *_ = self.parts[p]
        return self.g[k].at[0, layer, self.rows(p, self.at(away))]

    def load(self, p, away):
        return pltpu.make_async_copy(self.mine(p, away), self.term(p, away), self.load_sem.at[p, away % self.n])

    def remote(self, side, source, target, send_sem, recv_sem):
        return pltpu.make_async_remote_copy(
            src_ref=source, dst_ref=target, send_sem=send_sem, recv_sem=recv_sem, device_id={"dp": self.to[side]}, device_id_type=MESH
        )

    def sum_copy(self, p, side, left):
        away = left if side == 0 else -left
        source = self.mine(p, away) if self.hops[p][side] == left else self.term(p, away)
        at = (p, side, left - 1)
        return self.remote(side, source, self.came(p, side, left), self.send_sem.at[at], self.recv_sem.at[at])

    def gather_copy(self, p, side, hop, back):
        away = hop - back
        k, layer, *_ = self.parts[p]
        block = self.w_out[k].at[layer, self.rows(p, self.at(-away if side == 0 else away))]
        at = (p, side, hop - 1)
        return self.remote(side, block, block, self.gather_send_sem.at[at], self.gather_recv_sem.at[at])

    def live(self, side, hops):
        return [p for p in range(self.pieces) if self.hops[p][side] >= hops]

    def first_terms(self):
        for left in range(self.far, 0, -1):
            for order in zip(*([p for p in range(self.pieces) if self.hops[p][s] == left] for s in (0, 1)), strict=True):
                for s, p in enumerate(order):
                    self.sum_copy(p, s, left).start()

    def loaded(self):
        return [
            (p, away)
            for left in range(self.far - 1, -1, -1)
            for p in range(self.pieces)
            for away in sorted({left, -left})
            if left == 0 or self.hops[p][side_of(away)] > left
        ]

    def load_terms(self):
        for p, away in self.loaded():
            self.load(p, away).start()

    def states(self, k):
        mine, block = pl.ds(k * self.layers, self.layers), self.block(self.me)
        return [
            pltpu.make_async_copy(self.w[k].at[:, block], self.own.at[mine], self.state_sem.at[k, 0]),
            pltpu.make_async_copy(self.m[k], self.m_in.at[mine], self.state_sem.at[k, 1]),
            pltpu.make_async_copy(self.v[k], self.v_in.at[mine], self.state_sem.at[k, 2]),
        ]

    def load_states(self):
        for k in range(len(self.g)):
            for copy in self.states(k):
                copy.start()

    def pass_on(self):
        for left in range(self.far - 1, 0, -1):
            for order in zip(*(self.live(s, left + 1) for s in (0, 1)), strict=True):
                for s, p in enumerate(order):
                    away = left if s == 0 else -left
                    self.load(p, away).wait()
                    self.sum_copy(p, s, left + 1).wait_recv()
                    here, came = self.term(p, away), self.came(p, s, left + 1)

                    def add(r, here=here, came=came):
                        r = pl.ds(r, ROWS)
                        here[r, :] = (here[r, :].astype(jnp.float32) + came[r, :].astype(jnp.float32)).astype(jnp.bfloat16)

                    by_rows(self.parts[p][3], add)
                    self.sum_copy(p, s, left).start()

    def finish_sum(self, p):
        self.load(p, 0).wait()
        for s in (0, 1):
            self.sum_copy(p, s, 1).wait_recv()

        k, layer, first, count, _ = self.parts[p]

        def add(r):
            here = pl.ds(r, ROWS)
            parts = [ref[here, :].astype(jnp.float32) for ref in (self.term(p, 0), self.came(p, 0, 1), self.came(p, 1, 1))]
            self.total.at[k * self.layers + layer][pl.ds(first + r, ROWS), :] = (parts[0] + parts[1] + parts[2]).astype(jnp.bfloat16)

        by_rows(count, add)

    def sums_sent(self):
        for p in range(self.pieces):
            for s in (0, 1):
                for left in range(1, self.hops[p][s] + 1):
                    self.sum_copy(p, s, left).wait_send()

    def step(self, p):
        k, layer, first, count, _ = self.parts[p]
        if layer == 0 and first == 0:
            for copy in self.states(k):
                copy.wait()

        def take(r):
            rows = pl.ds(first + r, ROWS)
            w, m, v, g = (ref.at[k * self.layers + layer][rows, :] for ref in (self.own, self.m_in, self.v_in, self.total))
            new = adamw(w.astype(jnp.float32), m, v, g.astype(jnp.float32))
            self.w_out[k].at[layer][pl.ds(pl.multiple_of(self.me * self.block_rows + (first + r), ROWS), ROWS), :] = new[0]
            self.m_out[k].at[layer][rows, :] = new[1]
            self.v_out[k].at[layer][rows, :] = new[2]

        by_rows(count, take)
        for s in (0, 1):
            self.gather_copy(p, s, 1, 1).start()

    def gather(self):
        for hop in range(2, self.far + 1):
            order = [self.live(s, hop) for s in (0, 1)]
            for s in (0, 1):
                if hop == self.far - 1:
                    order[s].sort(key=lambda p, s=s: -self.hops[p][s])
            for pair in zip(*order, strict=True):
                for s, p in enumerate(pair):
                    self.gather_copy(p, s, hop - 1, 0).wait_recv()
                    self.gather_copy(p, s, hop, 1).start()
        for p in range(self.pieces):
            for s in (0, 1):
                self.gather_copy(p, s, self.hops[p][s], 0).wait_recv()
                for hop in range(1, self.hops[p][s] + 1):
                    self.gather_copy(p, s, hop, 1).wait_send()

    def greet(self):
        barrier = pltpu.get_barrier_semaphore()
        for neighbour in self.to:
            pl.semaphore_signal(barrier, inc=1, device_id={"dp": neighbour}, device_id_type=MESH)
        pl.semaphore_wait(barrier, 2)


def odd():
    return lax.rem(lax.axis_index("rep"), 2) == 1


def even():
    return lax.rem(lax.axis_index("rep"), 2) == 0


def early_kernel(n, count, *refs):
    refs = list(refs)
    take = lambda c: [refs.pop(0) for _ in range(c)]
    e, l = count
    g, w, m, v, late_g = take(e), take(e), take(e), take(e), take(l)
    results, late_total = [take(e) for _ in range(3)], refs.pop(0)
    me = lax.axis_index("dp")
    ring = Ring(n, me, EARLY_PIECES, g, w, m, v, results, take(6), take(6))
    terms, inbox = take(2)
    late = Ring(n, me, LATE_PIECES, late_g, None, None, None, (None,) * 3, (terms, inbox, late_total, None, None, None), take(6))

    ring.greet()

    @pl.when(odd())
    def _():
        late.first_terms()

    ring.first_terms()

    @pl.when(odd())
    def _():
        late.load_terms()

    ring.load_terms()
    ring.load_states()

    @pl.when(odd())
    def _():
        late.pass_on()
        for p in range(late.pieces):
            late.finish_sum(p)
        late.sums_sent()

    ring.pass_on()
    for p in range(ring.pieces):
        ring.finish_sum(p)
        ring.step(p)
    ring.gather()
    ring.sums_sent()


def late_kernel(n, count, *refs):
    refs = list(refs)
    take = lambda c: [refs.pop(0) for _ in range(c)]
    g, w, m, v, total = take(count), take(count), take(count), take(count), refs.pop(0)
    results = [take(count) for _ in range(3)]
    ring = Ring(n, lax.axis_index("dp"), LATE_PIECES, g, w, m, v, results, take(6), take(6))
    total_sem = refs.pop(0)
    ring.greet()

    @pl.when(even())
    def _():
        ring.first_terms()
        ring.load_terms()

    ring.load_states()

    @pl.when(odd())
    def _():
        copy = pltpu.make_async_copy(total, ring.total, total_sem)
        copy.start()
        copy.wait()

    @pl.when(even())
    def _():
        ring.pass_on()
        for p in range(ring.pieces):
            ring.finish_sum(p)
        ring.sums_sent()

    for p in range(ring.pieces):
        ring.step(p)
    ring.gather()


def put_kernel(count, *refs):
    sources, results, sem = refs[:count], refs[count:-1], refs[-1]
    copies = [pltpu.make_async_copy(a, b, sem.at[i]) for i, (a, b) in enumerate(zip(sources, results, strict=True))]
    for copy in copies:
        copy.start()
    for copy in copies:
        copy.wait()


def put(arrays):
    count = len(arrays)
    return pl.pallas_call(
        functools.partial(put_kernel, count),
        out_shape=[pltpu.HBM(one.shape, one.dtype) for one in arrays],
        in_specs=[VMEM] * count,
        out_specs=[HBM] * count,
        scratch_shapes=[DMA((count,))],
        compiler_params=pltpu.CompilerParams(vmem_limit_bytes=1 << 20),
    )(*arrays)


def solution(mesh):
    n = mesh.shape["dp"]

    def step(*arrays):
        g, w, m, v = (arrays[i : i + 3] for i in (0, 3, 6, 9))
        early, late = slice(0, 2), slice(2, 3)
        e, l = len(g[early]), len(g[late])
        layers = w[0].shape[0]
        vmem = lambda several: [pltpu.VMEM(one.shape, one.dtype) for one in several]
        early_shape, late_shape = m[early][0].shape[1:], m[late][0].shape[1:]

        *first, total = pl.pallas_call(
            functools.partial(early_kernel, n, (e, l)),
            out_shape=[*vmem((*w[early], *m[early], *v[early])), pltpu.VMEM((l * layers, *late_shape), jnp.bfloat16)],
            in_specs=[HBM] * (4 * e + l),
            out_specs=[VMEM] * (3 * e + 1),
            scratch_shapes=[
                *Ring.buffers(n, EARLY_PIECES, e, layers, early_shape, True),
                *Ring.sems(n, EARLY_PIECES, e, layers, early_shape),
                *Ring.buffers(n, LATE_PIECES, l, layers, late_shape, False),
                *Ring.sems(n, LATE_PIECES, l, layers, late_shape),
            ],
            compiler_params=pltpu.CompilerParams(collective_id=0, has_side_effects=True, vmem_limit_bytes=GRANT_EARLY),
        )(*g[early], *w[early], *m[early], *v[early], *g[late])
        *first, total = put([*first, total])
        second = pl.pallas_call(
            functools.partial(late_kernel, n, l),
            out_shape=vmem((*w[late], *m[late], *v[late])),
            in_specs=[HBM] * (4 * l + 1),
            out_specs=[VMEM] * (3 * l),
            scratch_shapes=[*Ring.buffers(n, LATE_PIECES, l, layers, late_shape, True), *Ring.sems(n, LATE_PIECES, l, layers, late_shape), DMA],
            compiler_params=pltpu.CompilerParams(collective_id=1, has_side_effects=True, vmem_limit_bytes=GRANT_LATE),
        )(*g[late], *w[late], *m[late], *v[late], total)
        second = put(second)
        return tuple(one for i in range(3) for one in (*first[i * e : (i + 1) * e], *second[i * l : (i + 1) * l]))

    all_of, cut = P(None, None, None), P(None, "dp", None)
    return jax.shard_map(
        step,
        mesh=mesh,
        in_specs=(P(("rep", "dp"), None, None, None),) * 3 + (all_of,) * 3 + (cut,) * 6,
        out_specs=(P("rep", None, None),) * 3 + (P("rep", "dp", None),) * 6,
        check_vma=False,
    )
```

```python
import functools

import jax
import jax.numpy as jnp
from jax import lax
from jax.experimental import pallas as pl
from jax.experimental.pallas import tpu as pltpu
from jax.sharding import PartitionSpec as P

MESH = pl.DeviceIdType.MESH
DMA = pltpu.SemaphoreType.DMA
HBM, VMEM = pl.BlockSpec(memory_space=pltpu.HBM), pl.BlockSpec(memory_space=pltpu.VMEM)
ROWS = 16
EARLY_PIECES, LATE_PIECES = 2, 4
GRANT_EARLY, GRANT_LATE = 57_000_000, 61_500_000


def adamw(w, m, v, g):
    m = 0.9 * m + 0.1 * g
    v = 0.95 * v + 0.05 * g * g
    step = m * lax.rsqrt(v + 1e-8) + 0.1 * w
    return (w - 0.02 * step).astype(jnp.bfloat16), m, v


def by_rows(count, body):
    lax.fori_loop(0, count // ROWS, lambda i, _: body(pl.multiple_of(i * ROWS, ROWS)), None)


def side_of(away):
    return 0 if away > 0 else 1


class Ring:
    def __init__(self, n, me, pieces, g, w, m, v, results, buffers, sems):
        self.n, self.me, self.g, self.w, self.m, self.v = n, me, g, w, m, v
        self.w_out, self.m_out, self.v_out = results
        self.terms, self.inbox, self.total, self.own, self.m_in, self.v_in = buffers
        self.load_sem, self.state_sem, self.send_sem, self.recv_sem, self.gather_send_sem, self.gather_recv_sem = sems
        self.to = [lax.rem(me + 1, n), lax.rem(me + n - 1, n)]
        self.layers = g[0].shape[1]
        self.block_rows = g[0].shape[2] // n
        self.parts = self.cut(len(g), self.layers, self.block_rows, pieces)
        self.pieces = len(self.parts)
        self.far = n // 2
        near = (n - 1) // 2
        self.hops = [(self.far, near) if turn == 0 else (near, self.far) for *_, turn in self.parts]

    @staticmethod
    def cut(weights, layers, rows, pieces):
        size = -(-rows // (pieces * ROWS)) * ROWS
        starts = range(0, rows, size)
        return [(k, layer, r, min(size, rows - r), (i + layer) % 2) for k in range(weights) for layer in range(layers) for i, r in enumerate(starts)]

    @classmethod
    def buffers(cls, n, pieces, weights, layers, shape, state):
        far = n // 2
        parts = cls.cut(weights, layers, shape[0], pieces)
        pieces, whole = len(parts), (weights * layers, *shape)
        shape = (parts[0][3], shape[1])
        data = [pltpu.VMEM((pieces, n, *shape), jnp.bfloat16), pltpu.VMEM((pieces, 2, far, *shape), jnp.bfloat16)]
        if state:
            data += [pltpu.VMEM(whole, t) for t in (jnp.bfloat16, jnp.bfloat16, jnp.float32, jnp.float32)]
        return data

    @classmethod
    def sems(cls, n, pieces, weights, layers, shape):
        far = n // 2
        pieces = len(cls.cut(weights, layers, shape[0], pieces))
        return [DMA((pieces, n)), DMA((weights, 3)), *(DMA((pieces, 2, far)) for _ in range(4))]

    def at(self, away):
        return lax.rem(self.me + (away + self.n), self.n)

    def block(self, owner):
        return pl.ds(pl.multiple_of(owner * self.block_rows, self.block_rows), self.block_rows)

    def rows(self, p, owner):
        _, _, first, count, _ = self.parts[p]
        return pl.ds(pl.multiple_of(owner * self.block_rows + first, ROWS), count)

    def term(self, p, away):
        return self.terms.at[p, away % self.n, pl.ds(0, self.parts[p][3])]

    def came(self, p, side, left):
        return self.inbox.at[p, side, left - 1, pl.ds(0, self.parts[p][3])]

    def mine(self, p, away):
        k, layer, *_ = self.parts[p]
        return self.g[k].at[0, layer, self.rows(p, self.at(away))]

    def load(self, p, away):
        return pltpu.make_async_copy(self.mine(p, away), self.term(p, away), self.load_sem.at[p, away % self.n])

    def remote(self, side, source, target, send_sem, recv_sem):
        return pltpu.make_async_remote_copy(
            src_ref=source, dst_ref=target, send_sem=send_sem, recv_sem=recv_sem, device_id={"dp": self.to[side]}, device_id_type=MESH
        )

    def sum_copy(self, p, side, left):
        away = left if side == 0 else -left
        source = self.mine(p, away) if self.hops[p][side] == left else self.term(p, away)
        at = (p, side, left - 1)
        return self.remote(side, source, self.came(p, side, left), self.send_sem.at[at], self.recv_sem.at[at])

    def gather_copy(self, p, side, hop, back):
        away = hop - back
        k, layer, *_ = self.parts[p]
        block = self.w_out[k].at[layer, self.rows(p, self.at(-away if side == 0 else away))]
        at = (p, side, hop - 1)
        return self.remote(side, block, block, self.gather_send_sem.at[at], self.gather_recv_sem.at[at])

    def live(self, side, hops):
        return [p for p in range(self.pieces) if self.hops[p][side] >= hops]

    def first_terms(self):
        for left in range(self.far, 0, -1):
            for order in zip(*([p for p in range(self.pieces) if self.hops[p][s] == left] for s in (0, 1)), strict=True):
                for s, p in enumerate(order):
                    self.sum_copy(p, s, left).start()

    def loaded(self):
        return [
            (p, away)
            for left in range(self.far - 1, -1, -1)
            for p in range(self.pieces)
            for away in sorted({left, -left})
            if left == 0 or self.hops[p][side_of(away)] > left
        ]

    def load_terms(self):
        for p, away in self.loaded():
            self.load(p, away).start()

    def states(self, k):
        mine, block = pl.ds(k * self.layers, self.layers), self.block(self.me)
        return [
            pltpu.make_async_copy(self.w[k].at[:, block], self.own.at[mine], self.state_sem.at[k, 0]),
            pltpu.make_async_copy(self.m[k], self.m_in.at[mine], self.state_sem.at[k, 1]),
            pltpu.make_async_copy(self.v[k], self.v_in.at[mine], self.state_sem.at[k, 2]),
        ]

    def load_states(self):
        for k in range(len(self.g)):
            for copy in self.states(k):
                copy.start()

    def pass_on(self):
        for left in range(self.far - 1, 0, -1):
            for order in zip(*(self.live(s, left + 1) for s in (0, 1)), strict=True):
                for s, p in enumerate(order):
                    away = left if s == 0 else -left
                    self.load(p, away).wait()
                    self.sum_copy(p, s, left + 1).wait_recv()
                    here, came = self.term(p, away), self.came(p, s, left + 1)

                    def add(r, here=here, came=came):
                        r = pl.ds(r, ROWS)
                        here[r, :] = (here[r, :].astype(jnp.float32) + came[r, :].astype(jnp.float32)).astype(jnp.bfloat16)

                    by_rows(self.parts[p][3], add)
                    self.sum_copy(p, s, left).start()

    def finish_sum(self, p):
        self.load(p, 0).wait()
        for s in (0, 1):
            self.sum_copy(p, s, 1).wait_recv()

        k, layer, first, count, _ = self.parts[p]

        def add(r):
            here = pl.ds(r, ROWS)
            parts = [ref[here, :].astype(jnp.float32) for ref in (self.term(p, 0), self.came(p, 0, 1), self.came(p, 1, 1))]
            self.total.at[k * self.layers + layer][pl.ds(first + r, ROWS), :] = (parts[0] + parts[1] + parts[2]).astype(jnp.bfloat16)

        by_rows(count, add)

    def sums_sent(self):
        for p in range(self.pieces):
            for s in (0, 1):
                for left in range(1, self.hops[p][s] + 1):
                    self.sum_copy(p, s, left).wait_send()

    def step(self, p):
        k, layer, first, count, _ = self.parts[p]
        if layer == 0 and first == 0:
            for copy in self.states(k):
                copy.wait()

        def take(r):
            rows = pl.ds(first + r, ROWS)
            w, m, v, g = (ref.at[k * self.layers + layer][rows, :] for ref in (self.own, self.m_in, self.v_in, self.total))
            new = adamw(w.astype(jnp.float32), m, v, g.astype(jnp.float32))
            self.w_out[k].at[layer][pl.ds(pl.multiple_of(self.me * self.block_rows + (first + r), ROWS), ROWS), :] = new[0]
            self.m_out[k].at[layer][rows, :] = new[1]
            self.v_out[k].at[layer][rows, :] = new[2]

        by_rows(count, take)
        for s in (0, 1):
            self.gather_copy(p, s, 1, 1).start()

    def gather(self):
        for hop in range(2, self.far + 1):
            order = [self.live(s, hop) for s in (0, 1)]
            for s in (0, 1):
                if hop == self.far - 1:
                    order[s].sort(key=lambda p, s=s: -self.hops[p][s])
            for pair in zip(*order, strict=True):
                for s, p in enumerate(pair):
                    self.gather_copy(p, s, hop - 1, 0).wait_recv()
                    self.gather_copy(p, s, hop, 1).start()
        for p in range(self.pieces):
            for s in (0, 1):
                self.gather_copy(p, s, self.hops[p][s], 0).wait_recv()
                for hop in range(1, self.hops[p][s] + 1):
                    self.gather_copy(p, s, hop, 1).wait_send()

    def greet(self):
        barrier = pltpu.get_barrier_semaphore()
        for neighbour in self.to:
            pl.semaphore_signal(barrier, inc=1, device_id={"dp": neighbour}, device_id_type=MESH)
        pl.semaphore_wait(barrier, 2)


def odd():
    return lax.rem(lax.axis_index("rep"), 2) == 1


def even():
    return lax.rem(lax.axis_index("rep"), 2) == 0


def early_kernel(n, count, *refs):
    refs = list(refs)
    take = lambda c: [refs.pop(0) for _ in range(c)]
    e, l = count
    g, w, m, v, late_g = take(e), take(e), take(e), take(e), take(l)
    results, late_total = [take(e) for _ in range(3)], refs.pop(0)
    me = lax.axis_index("dp")
    ring = Ring(n, me, EARLY_PIECES, g, w, m, v, results, take(6), take(6))
    terms, inbox = take(2)
    late = Ring(n, me, LATE_PIECES, late_g, None, None, None, (None,) * 3, (terms, inbox, late_total, None, None, None), take(6))

    ring.greet()

    @pl.when(odd())
    def _():
        late.first_terms()

    ring.first_terms()

    @pl.when(odd())
    def _():
        late.load_terms()

    ring.load_terms()
    ring.load_states()

    @pl.when(odd())
    def _():
        late.pass_on()
        for p in range(late.pieces):
            late.finish_sum(p)
        late.sums_sent()

    ring.pass_on()
    for p in range(ring.pieces):
        ring.finish_sum(p)
        ring.step(p)
    ring.gather()
    ring.sums_sent()


def late_kernel(n, count, *refs):
    refs = list(refs)
    take = lambda c: [refs.pop(0) for _ in range(c)]
    g, w, m, v, total = take(count), take(count), take(count), take(count), refs.pop(0)
    results = [take(count) for _ in range(3)]
    ring = Ring(n, lax.axis_index("dp"), LATE_PIECES, g, w, m, v, results, take(6), take(6))
    total_sem = refs.pop(0)
    ring.greet()

    @pl.when(even())
    def _():
        ring.first_terms()
        ring.load_terms()

    ring.load_states()

    @pl.when(odd())
    def _():
        copy = pltpu.make_async_copy(total, ring.total, total_sem)
        copy.start()
        copy.wait()

    pl.when(even())(ring.pass_on)
    for p in range(ring.pieces):
        pl.when(even())(functools.partial(ring.finish_sum, p))
        ring.step(p)
    ring.gather()
    pl.when(even())(ring.sums_sent)


def put_kernel(count, *refs):
    sources, results, sem = refs[:count], refs[count:-1], refs[-1]
    copies = [pltpu.make_async_copy(a, b, sem.at[i]) for i, (a, b) in enumerate(zip(sources, results, strict=True))]
    for copy in copies:
        copy.start()
    for copy in copies:
        copy.wait()


def put(arrays):
    count = len(arrays)
    return pl.pallas_call(
        functools.partial(put_kernel, count),
        out_shape=[pltpu.HBM(one.shape, one.dtype) for one in arrays],
        in_specs=[VMEM] * count,
        out_specs=[HBM] * count,
        scratch_shapes=[DMA((count,))],
        compiler_params=pltpu.CompilerParams(vmem_limit_bytes=1 << 20),
    )(*arrays)


def solution(mesh):
    n = mesh.shape["dp"]

    def step(*arrays):
        g, w, m, v = (arrays[i : i + 3] for i in (0, 3, 6, 9))
        early, late = slice(0, 2), slice(2, 3)
        e, l = len(g[early]), len(g[late])
        layers = w[0].shape[0]
        vmem = lambda several: [pltpu.VMEM(one.shape, one.dtype) for one in several]
        early_shape, late_shape = m[early][0].shape[1:], m[late][0].shape[1:]

        *first, total = pl.pallas_call(
            functools.partial(early_kernel, n, (e, l)),
            out_shape=[*vmem((*w[early], *m[early], *v[early])), pltpu.VMEM((l * layers, *late_shape), jnp.bfloat16)],
            in_specs=[HBM] * (4 * e + l),
            out_specs=[VMEM] * (3 * e + 1),
            scratch_shapes=[
                *Ring.buffers(n, EARLY_PIECES, e, layers, early_shape, True),
                *Ring.sems(n, EARLY_PIECES, e, layers, early_shape),
                *Ring.buffers(n, LATE_PIECES, l, layers, late_shape, False),
                *Ring.sems(n, LATE_PIECES, l, layers, late_shape),
            ],
            compiler_params=pltpu.CompilerParams(collective_id=0, has_side_effects=True, vmem_limit_bytes=GRANT_EARLY),
        )(*g[early], *w[early], *m[early], *v[early], *g[late])
        *first, total = put([*first, total])
        second = pl.pallas_call(
            functools.partial(late_kernel, n, l),
            out_shape=vmem((*w[late], *m[late], *v[late])),
            in_specs=[HBM] * (4 * l + 1),
            out_specs=[VMEM] * (3 * l),
            scratch_shapes=[*Ring.buffers(n, LATE_PIECES, l, layers, late_shape, True), *Ring.sems(n, LATE_PIECES, l, layers, late_shape), DMA],
            compiler_params=pltpu.CompilerParams(collective_id=1, has_side_effects=True, vmem_limit_bytes=GRANT_LATE),
        )(*g[late], *w[late], *m[late], *v[late], total)
        second = put(second)
        return tuple(one for i in range(3) for one in (*first[i * e : (i + 1) * e], *second[i * l : (i + 1) * l]))

    all_of, cut = P(None, None, None), P(None, "dp", None)
    return jax.shard_map(
        step,
        mesh=mesh,
        in_specs=(P(("rep", "dp"), None, None, None),) * 3 + (all_of,) * 3 + (cut,) * 6,
        out_specs=(P("rep", None, None),) * 3 + (P("rep", "dp", None),) * 6,
        check_vma=False,
    )
```

```python
import functools

import jax
import jax.numpy as jnp
from jax import lax
from jax.experimental import pallas as pl
from jax.experimental.pallas import tpu as pltpu
from jax.sharding import PartitionSpec as P

MESH = pl.DeviceIdType.MESH
DMA = pltpu.SemaphoreType.DMA
HBM, VMEM = pl.BlockSpec(memory_space=pltpu.HBM), pl.BlockSpec(memory_space=pltpu.VMEM)
ROWS = 16
EARLY_PIECES, LATE_PIECES = 1, 3
GRANT_EARLY, GRANT_LATE = 57_000_000, 61_500_000


def adamw(w, m, v, g):
    m = 0.9 * m + 0.1 * g
    v = 0.95 * v + 0.05 * g * g
    step = m * lax.rsqrt(v + 1e-8) + 0.1 * w
    return (w - 0.02 * step).astype(jnp.bfloat16), m, v


def by_rows(count, body):
    lax.fori_loop(0, count // ROWS, lambda i, _: body(pl.multiple_of(i * ROWS, ROWS)), None)


class Ring:
    def __init__(self, n, me, shape, pieces, g, w, m, v, results, buffers, sems):
        self.n, self.me, self.g, self.w, self.m, self.v = n, me, g, w, m, v
        self.w_out, self.m_out, self.v_out = results
        self.terms, self.inbox, self.total, self.own, self.m_in, self.v_in = buffers
        self.load_sem, self.state_sem, self.send_sem, self.recv_sem = sems
        self.to = [lax.rem(me + 1, n), lax.rem(me + n - 1, n)]
        weights, self.layers, self.block_rows, _ = shape
        self.parts, self.hops, self.place, _, self.message, _ = self.cut(n, pieces, shape)
        self.pieces = len(self.parts)
        self.far = n // 2
        self.loads_over = set()

    @staticmethod
    def cut(n, pieces, shape):
        weights, layers, rows, _ = shape
        size = -(-rows // (pieces * ROWS)) * ROWS
        parts, hops, place, message = [], [], {}, {}
        end = [0, 0]
        for k in range(weights):
            for layer in range(layers):
                for i, r in enumerate(range(0, rows, size)):
                    p, count = len(parts), min(size, rows - r)
                    parts.append((k, layer, r, count))
                    ways = (n // 2, (n - 1) // 2)
                    hops.append(ways if (i + layer) % 2 == 0 else ways[::-1])
                    for s in (0, 1):
                        for left in range(1, hops[p][s] + 1):
                            place[p, s, left] = end[s]
                            end[s] += count
                            message[p, s, left] = len(message)
        assert end[0] == end[1]
        return parts, hops, place, end[0], message, len(message)

    @classmethod
    def scratch(cls, n, pieces, shape, state):
        weights, layers, rows, columns = shape
        _, _, _, inbox_rows, _, messages = cls.cut(n, pieces, shape)
        whole = (weights * layers, rows, columns)
        data = [pltpu.VMEM((n, *whole), jnp.bfloat16), pltpu.VMEM((2, inbox_rows, columns), jnp.bfloat16)]
        if state:
            data += [pltpu.VMEM(whole, t) for t in (jnp.bfloat16, jnp.bfloat16, jnp.float32, jnp.float32)]
        return [*data, DMA((n,)), DMA((3,)), DMA((2,)), DMA((messages,))]

    def at(self, away):
        return lax.rem(self.me + (away + self.n), self.n)

    def block(self, owner):
        return pl.ds(pl.multiple_of(owner * self.block_rows, self.block_rows), self.block_rows)

    def rows(self, p, owner):
        _, _, first, count = self.parts[p]
        return pl.ds(pl.multiple_of(owner * self.block_rows + first, ROWS), count)

    def matrix(self, p):
        k, layer, *_ = self.parts[p]
        return k * self.layers + layer

    def term(self, p, away):
        _, _, first, count = self.parts[p]
        return self.terms.at[away % self.n, self.matrix(p), pl.ds(first, count)]

    def came(self, p, side, left):
        return self.inbox.at[side, pl.ds(self.place[p, side, left], self.parts[p][3])]

    def load_terms(self):
        for left in range(self.far - 1, -1, -1):
            for away in sorted({left, -left}):
                for k, g in enumerate(self.g):
                    target = self.terms.at[away % self.n, pl.ds(k * self.layers, self.layers)]
                    pltpu.make_async_copy(g.at[0, :, self.block(self.at(away))], target, self.load_sem.at[away % self.n]).start()

    def loaded(self, away):
        if away not in self.loads_over:
            self.loads_over.add(away)
            whole = self.terms.at[away % self.n]
            pltpu.make_async_copy(whole, whole, self.load_sem.at[away % self.n]).wait()

    def load_states(self):
        for k in range(len(self.g)):
            mine = pl.ds(k * self.layers, self.layers)
            sources = (self.w[k].at[:, self.block(self.me)], self.m[k], self.v[k])
            for i, (source, target) in enumerate(zip(sources, (self.own, self.m_in, self.v_in), strict=True)):
                pltpu.make_async_copy(source, target.at[mine], self.state_sem.at[i]).start()

    def states_loaded(self):
        for i, whole in enumerate((self.own, self.m_in, self.v_in)):
            pltpu.make_async_copy(whole, whole, self.state_sem.at[i]).wait()

    def remote(self, side, source, target, recv_sem):
        return pltpu.make_async_remote_copy(
            src_ref=source,
            dst_ref=target,
            send_sem=self.send_sem.at[side],
            recv_sem=self.recv_sem.at[recv_sem],
            device_id={"dp": self.to[side]},
            device_id_type=MESH,
        )

    def sum_copy(self, p, side, left):
        away = left if side == 0 else -left
        if self.hops[p][side] == left:
            k, layer, *_ = self.parts[p]
            source = self.g[k].at[0, layer, self.rows(p, self.at(away))]
        else:
            source = self.term(p, away)
        return self.remote(side, source, self.came(p, side, left), self.message[p, side, left])

    def gather_copy(self, p, side, hop, back):
        away = hop - back
        k, layer, *_ = self.parts[p]
        block = self.w_out[k].at[layer, self.rows(p, self.at(-away if side == 0 else away))]
        return self.remote(side, block, block, self.message[p, side, self.hops[p][side] + 1 - hop])

    def live(self, side, hops):
        return [p for p in range(self.pieces) if self.hops[p][side] >= hops]

    def first_terms(self):
        for left in range(self.far, 0, -1):
            for order in zip(*([p for p in range(self.pieces) if self.hops[p][s] == left] for s in (0, 1)), strict=True):
                for s, p in enumerate(order):
                    self.sum_copy(p, s, left).start()

    def pass_on(self):
        for left in range(self.far - 1, 0, -1):
            for order in zip(*(self.live(s, left + 1) for s in (0, 1)), strict=True):
                for s, p in enumerate(order):
                    away = left if s == 0 else -left
                    self.loaded(away)
                    self.sum_copy(p, s, left + 1).wait_recv()
                    here, came = self.term(p, away), self.came(p, s, left + 1)

                    def add(r, here=here, came=came):
                        r = pl.ds(r, ROWS)
                        here[r, :] = (here[r, :].astype(jnp.float32) + came[r, :].astype(jnp.float32)).astype(jnp.bfloat16)

                    by_rows(self.parts[p][3], add)
                    self.sum_copy(p, s, left).start()

    def finish_sum(self, p):
        self.loaded(0)
        for s in (0, 1):
            self.sum_copy(p, s, 1).wait_recv()
        _, _, first, count = self.parts[p]

        def add(r):
            here = pl.ds(r, ROWS)
            parts = [ref[here, :].astype(jnp.float32) for ref in (self.term(p, 0), self.came(p, 0, 1), self.came(p, 1, 1))]
            self.total.at[self.matrix(p)][pl.ds(first + r, ROWS), :] = (parts[0] + parts[1] + parts[2]).astype(jnp.bfloat16)

        by_rows(count, add)

    def step(self, p):
        k, layer, first, count = self.parts[p]

        def take(r):
            rows = pl.ds(first + r, ROWS)
            w, m, v, g = (ref.at[self.matrix(p)][rows, :] for ref in (self.own, self.m_in, self.v_in, self.total))
            new = adamw(w.astype(jnp.float32), m, v, g.astype(jnp.float32))
            self.w_out[k].at[layer][pl.ds(pl.multiple_of(self.me * self.block_rows + (first + r), ROWS), ROWS), :] = new[0]
            self.m_out[k].at[layer][rows, :] = new[1]
            self.v_out[k].at[layer][rows, :] = new[2]

        by_rows(count, take)
        for s in (0, 1):
            self.gather_copy(p, s, 1, 1).start()

    def gather(self):
        for hop in range(2, self.far + 1):
            order = [self.live(s, hop) for s in (0, 1)]
            for s in (0, 1):
                if hop == self.far - 1:
                    order[s].sort(key=lambda p, s=s: -self.hops[p][s])
            for pair in zip(*order, strict=True):
                for s, p in enumerate(pair):
                    self.gather_copy(p, s, hop - 1, 0).wait_recv()
                    self.gather_copy(p, s, hop, 1).start()
        for hop in (self.far - 1, self.far):
            for p in range(self.pieces):
                for s in (0, 1):
                    if self.hops[p][s] == hop:
                        self.gather_copy(p, s, hop, 0).wait_recv()

    def all_sent(self, phases):
        for s in (0, 1):
            whole = self.inbox if phases == 2 else self.inbox.at[s]
            pltpu.make_async_copy(whole, whole, self.send_sem.at[s]).wait()

    def greet(self):
        barrier = pltpu.get_barrier_semaphore()
        for neighbour in self.to:
            pl.semaphore_signal(barrier, inc=1, device_id={"dp": neighbour}, device_id_type=MESH)
        pl.semaphore_wait(barrier, 2)


def odd():
    return lax.rem(lax.axis_index("rep"), 2) == 1


def even():
    return lax.rem(lax.axis_index("rep"), 2) == 0


def early_kernel(n, shape, late_shape, *refs):
    refs = list(refs)
    take = lambda c: [refs.pop(0) for _ in range(c)]
    e, l = shape[0], late_shape[0]
    g, w, m, v, late_g = take(e), take(e), take(e), take(e), take(l)
    results, late_total = [take(e) for _ in range(3)], refs.pop(0)
    me = lax.axis_index("dp")
    ring = Ring(n, me, shape, EARLY_PIECES, g, w, m, v, results, take(6), take(4))
    held = (*take(2), late_total, None, None, None)
    late = Ring(n, me, late_shape, LATE_PIECES, late_g, None, None, None, (None,) * 3, held, take(4))

    ring.greet()

    @pl.when(odd())
    def _():
        late.first_terms()

    ring.first_terms()

    @pl.when(odd())
    def _():
        late.load_terms()

    ring.load_terms()
    ring.load_states()

    @pl.when(odd())
    def _():
        late.pass_on()
        for p in range(late.pieces):
            late.finish_sum(p)

    ring.pass_on()
    ring.states_loaded()
    for p in range(ring.pieces):
        ring.finish_sum(p)
        ring.step(p)
    ring.gather()
    ring.all_sent(2)
    pl.when(odd())(functools.partial(late.all_sent, 1))


def late_kernel(n, shape, *refs):
    refs = list(refs)
    take = lambda c: [refs.pop(0) for _ in range(c)]
    count = shape[0]
    g, w, m, v, total = take(count), take(count), take(count), take(count), refs.pop(0)
    results = [take(count) for _ in range(3)]
    ring = Ring(n, lax.axis_index("dp"), shape, LATE_PIECES, g, w, m, v, results, take(6), take(4))
    total_sem = refs.pop(0)
    ring.greet()

    @pl.when(even())
    def _():
        ring.first_terms()
        ring.load_terms()

    ring.load_states()

    @pl.when(odd())
    def _():
        copy = pltpu.make_async_copy(total, ring.total, total_sem)
        copy.start()
        copy.wait()

    pl.when(even())(ring.pass_on)
    ring.states_loaded()
    pl.when(even())(functools.partial(ring.loaded, 0))
    for p in range(ring.pieces):
        pl.when(even())(functools.partial(ring.finish_sum, p))
        ring.step(p)
    ring.gather()
    pl.when(even())(functools.partial(ring.all_sent, 2))
    pl.when(odd())(functools.partial(ring.all_sent, 1))


def put_kernel(count, *refs):
    sources, results, sem = refs[:count], refs[count:-1], refs[-1]
    copies = [pltpu.make_async_copy(a, b, sem.at[i]) for i, (a, b) in enumerate(zip(sources, results, strict=True))]
    for copy in copies:
        copy.start()
    for copy in copies:
        copy.wait()


def put(arrays):
    count = len(arrays)
    return pl.pallas_call(
        functools.partial(put_kernel, count),
        out_shape=[pltpu.HBM(one.shape, one.dtype) for one in arrays],
        in_specs=[VMEM] * count,
        out_specs=[HBM] * count,
        scratch_shapes=[DMA((count,))],
        compiler_params=pltpu.CompilerParams(vmem_limit_bytes=1 << 20),
    )(*arrays)


def solution(mesh):
    n = mesh.shape["dp"]

    def step(*arrays):
        g, w, m, v = (arrays[i : i + 3] for i in (0, 3, 6, 9))
        early, late = slice(0, 2), slice(2, 3)
        e, l = len(g[early]), len(g[late])
        vmem = lambda several: [pltpu.VMEM(one.shape, one.dtype) for one in several]
        early_shape, late_shape = (e, *m[early][0].shape), (l, *m[late][0].shape)

        *first, total = pl.pallas_call(
            functools.partial(early_kernel, n, early_shape, late_shape),
            out_shape=[*vmem((*w[early], *m[early], *v[early])), pltpu.VMEM((l * late_shape[1], *late_shape[2:]), jnp.bfloat16)],
            in_specs=[HBM] * (4 * e + l),
            out_specs=[VMEM] * (3 * e + 1),
            scratch_shapes=[
                *Ring.scratch(n, EARLY_PIECES, early_shape, True),
                *Ring.scratch(n, LATE_PIECES, late_shape, False),
            ],
            compiler_params=pltpu.CompilerParams(collective_id=0, has_side_effects=True, vmem_limit_bytes=GRANT_EARLY),
        )(*g[early], *w[early], *m[early], *v[early], *g[late])
        *first, total = put([*first, total])
        second = pl.pallas_call(
            functools.partial(late_kernel, n, late_shape),
            out_shape=vmem((*w[late], *m[late], *v[late])),
            in_specs=[HBM] * (4 * l + 1),
            out_specs=[VMEM] * (3 * l),
            scratch_shapes=[*Ring.scratch(n, LATE_PIECES, late_shape, True), DMA],
            compiler_params=pltpu.CompilerParams(collective_id=1, has_side_effects=True, vmem_limit_bytes=GRANT_LATE),
        )(*g[late], *w[late], *m[late], *v[late], total)
        second = put(second)
        return tuple(one for i in range(3) for one in (*first[i * e : (i + 1) * e], *second[i * l : (i + 1) * l]))

    all_of, cut = P(None, None, None), P(None, "dp", None)
    return jax.shard_map(
        step,
        mesh=mesh,
        in_specs=(P(("rep", "dp"), None, None, None),) * 3 + (all_of,) * 3 + (cut,) * 6,
        out_specs=(P("rep", None, None),) * 3 + (P("rep", "dp", None),) * 6,
        check_vma=False,
    )
```

```python
import functools

import jax
import jax.numpy as jnp
from jax import lax
from jax.experimental import pallas as pl
from jax.experimental.pallas import tpu as pltpu
from jax.sharding import PartitionSpec as P

MESH = pl.DeviceIdType.MESH
DMA = pltpu.SemaphoreType.DMA
HBM, VMEM = pl.BlockSpec(memory_space=pltpu.HBM), pl.BlockSpec(memory_space=pltpu.VMEM)
ROWS = 16
EARLY_PIECES, LATE_PIECES = 1, 4
GRANT_EARLY, GRANT_LATE = 57_000_000, 61_500_000


def adamw(w, m, v, g):
    m = 0.9 * m + 0.1 * g
    v = 0.95 * v + 0.05 * g * g
    step = m * lax.rsqrt(v + 1e-8) + 0.1 * w
    return (w - 0.02 * step).astype(jnp.bfloat16), m, v


def by_rows(count, body):
    lax.fori_loop(0, count // ROWS, lambda i, _: body(pl.multiple_of(i * ROWS, ROWS)), None)


class Ring:
    def __init__(self, n, me, shape, pieces, g, w, m, v, results, buffers, sems):
        self.n, self.me, self.g, self.w, self.m, self.v = n, me, g, w, m, v
        self.w_out, self.m_out, self.v_out = results
        self.terms, self.inbox, self.total, self.own, self.m_in, self.v_in = buffers
        self.load_sem, self.state_sem, self.send_sem, self.recv_sem = sems
        self.to = [lax.rem(me + 1, n), lax.rem(me + n - 1, n)]
        weights, self.layers, self.block_rows, _ = shape
        self.parts, self.hops, self.place, _, self.message, _ = self.cut(n, pieces, shape)
        self.pieces = len(self.parts)
        self.far = n // 2
        self.loads_over = set()

    @staticmethod
    def cut(n, pieces, shape):
        weights, layers, rows, _ = shape
        size = -(-rows // (pieces * ROWS)) * ROWS
        parts, hops, place, message = [], [], {}, {}
        end = [0, 0]
        for k in range(weights):
            for layer in range(layers):
                for i, r in enumerate(range(0, rows, size)):
                    p, count = len(parts), min(size, rows - r)
                    parts.append((k, layer, r, count))
                    ways = (n // 2, (n - 1) // 2)
                    hops.append(ways if (i + layer) % 2 == 0 else ways[::-1])
                    for s in (0, 1):
                        for left in range(1, hops[p][s] + 1):
                            place[p, s, left] = end[s]
                            end[s] += count
                            message[p, s, left] = len(message)
        assert end[0] == end[1]
        return parts, hops, place, end[0], message, len(message)

    @classmethod
    def scratch(cls, n, pieces, shape, state):
        weights, layers, rows, columns = shape
        _, _, _, inbox_rows, _, messages = cls.cut(n, pieces, shape)
        whole = (weights * layers, rows, columns)
        data = [pltpu.VMEM((n, *whole), jnp.bfloat16), pltpu.VMEM((2, inbox_rows, columns), jnp.bfloat16)]
        if state:
            data += [pltpu.VMEM(whole, t) for t in (jnp.bfloat16, jnp.bfloat16, jnp.float32, jnp.float32)]
        return [*data, DMA((n,)), DMA((3,)), DMA((2,)), DMA((messages,))]

    def at(self, away):
        return lax.rem(self.me + (away + self.n), self.n)

    def block(self, owner):
        return pl.ds(pl.multiple_of(owner * self.block_rows, self.block_rows), self.block_rows)

    def rows(self, p, owner):
        _, _, first, count = self.parts[p]
        return pl.ds(pl.multiple_of(owner * self.block_rows + first, ROWS), count)

    def matrix(self, p):
        k, layer, *_ = self.parts[p]
        return k * self.layers + layer

    def term(self, p, away):
        _, _, first, count = self.parts[p]
        return self.terms.at[away % self.n, self.matrix(p), pl.ds(first, count)]

    def came(self, p, side, left):
        return self.inbox.at[side, pl.ds(self.place[p, side, left], self.parts[p][3])]

    def load_terms(self):
        for left in range(self.far - 1, -1, -1):
            for away in sorted({left, -left}):
                for k, g in enumerate(self.g):
                    target = self.terms.at[away % self.n, pl.ds(k * self.layers, self.layers)]
                    pltpu.make_async_copy(g.at[0, :, self.block(self.at(away))], target, self.load_sem.at[away % self.n]).start()

    def loaded(self, away):
        if away not in self.loads_over:
            self.loads_over.add(away)
            whole = self.terms.at[away % self.n]
            pltpu.make_async_copy(whole, whole, self.load_sem.at[away % self.n]).wait()

    def load_states(self):
        for k in range(len(self.g)):
            mine = pl.ds(k * self.layers, self.layers)
            sources = (self.w[k].at[:, self.block(self.me)], self.m[k], self.v[k])
            for i, (source, target) in enumerate(zip(sources, (self.own, self.m_in, self.v_in), strict=True)):
                pltpu.make_async_copy(source, target.at[mine], self.state_sem.at[i]).start()

    def states_loaded(self):
        for i, whole in enumerate((self.own, self.m_in, self.v_in)):
            pltpu.make_async_copy(whole, whole, self.state_sem.at[i]).wait()

    def remote(self, side, source, target, recv_sem):
        return pltpu.make_async_remote_copy(
            src_ref=source,
            dst_ref=target,
            send_sem=self.send_sem.at[side],
            recv_sem=self.recv_sem.at[recv_sem],
            device_id={"dp": self.to[side]},
            device_id_type=MESH,
        )

    def sum_copy(self, p, side, left):
        away = left if side == 0 else -left
        if self.hops[p][side] == left:
            k, layer, *_ = self.parts[p]
            source = self.g[k].at[0, layer, self.rows(p, self.at(away))]
        else:
            source = self.term(p, away)
        return self.remote(side, source, self.came(p, side, left), self.message[p, side, left])

    def gather_copy(self, p, side, hop, back):
        away = hop - back
        k, layer, *_ = self.parts[p]
        block = self.w_out[k].at[layer, self.rows(p, self.at(-away if side == 0 else away))]
        return self.remote(side, block, block, self.message[p, side, self.hops[p][side] + 1 - hop])

    def live(self, side, hops):
        return [p for p in range(self.pieces) if self.hops[p][side] >= hops]

    def first_terms(self):
        for left in range(self.far, 0, -1):
            for order in zip(*([p for p in range(self.pieces) if self.hops[p][s] == left] for s in (0, 1)), strict=True):
                for s, p in enumerate(order):
                    self.sum_copy(p, s, left).start()

    def pass_on(self):
        for left in range(self.far - 1, 0, -1):
            for order in zip(*(self.live(s, left + 1) for s in (0, 1)), strict=True):
                for s, p in enumerate(order):
                    away = left if s == 0 else -left
                    self.loaded(away)
                    self.sum_copy(p, s, left + 1).wait_recv()
                    here, came = self.term(p, away), self.came(p, s, left + 1)

                    def add(r, here=here, came=came):
                        r = pl.ds(r, ROWS)
                        here[r, :] = (here[r, :].astype(jnp.float32) + came[r, :].astype(jnp.float32)).astype(jnp.bfloat16)

                    by_rows(self.parts[p][3], add)
                    self.sum_copy(p, s, left).start()

    def finish_sum(self, p):
        self.loaded(0)
        for s in (0, 1):
            self.sum_copy(p, s, 1).wait_recv()
        _, _, first, count = self.parts[p]

        def add(r):
            here = pl.ds(r, ROWS)
            parts = [ref[here, :].astype(jnp.float32) for ref in (self.term(p, 0), self.came(p, 0, 1), self.came(p, 1, 1))]
            self.total.at[self.matrix(p)][pl.ds(first + r, ROWS), :] = (parts[0] + parts[1] + parts[2]).astype(jnp.bfloat16)

        by_rows(count, add)

    def step(self, p):
        k, layer, first, count = self.parts[p]

        def take(r):
            rows = pl.ds(first + r, ROWS)
            w, m, v, g = (ref.at[self.matrix(p)][rows, :] for ref in (self.own, self.m_in, self.v_in, self.total))
            new = adamw(w.astype(jnp.float32), m, v, g.astype(jnp.float32))
            self.w_out[k].at[layer][pl.ds(pl.multiple_of(self.me * self.block_rows + (first + r), ROWS), ROWS), :] = new[0]
            self.m_out[k].at[layer][rows, :] = new[1]
            self.v_out[k].at[layer][rows, :] = new[2]

        by_rows(count, take)
        for s in (0, 1):
            self.gather_copy(p, s, 1, 1).start()

    def gather(self):
        for hop in range(2, self.far + 1):
            order = [self.live(s, hop) for s in (0, 1)]
            for s in (0, 1):
                if hop == self.far - 1:
                    order[s].sort(key=lambda p, s=s: -self.hops[p][s])
            for pair in zip(*order, strict=True):
                for s, p in enumerate(pair):
                    self.gather_copy(p, s, hop - 1, 0).wait_recv()
                    self.gather_copy(p, s, hop, 1).start()
        for hop in (self.far - 1, self.far):
            for p in range(self.pieces):
                for s in (0, 1):
                    if self.hops[p][s] == hop:
                        self.gather_copy(p, s, hop, 0).wait_recv()

    def all_sent(self, phases):
        for s in (0, 1):
            whole = self.inbox if phases == 2 else self.inbox.at[s]
            pltpu.make_async_copy(whole, whole, self.send_sem.at[s]).wait()

    def greet(self):
        barrier = pltpu.get_barrier_semaphore()
        for neighbour in self.to:
            pl.semaphore_signal(barrier, inc=1, device_id={"dp": neighbour}, device_id_type=MESH)
        pl.semaphore_wait(barrier, 2)


def odd():
    return lax.rem(lax.axis_index("rep"), 2) == 0


def even():
    return lax.rem(lax.axis_index("rep"), 2) == 1


def early_kernel(n, shape, late_shape, *refs):
    refs = list(refs)
    take = lambda c: [refs.pop(0) for _ in range(c)]
    e, l = shape[0], late_shape[0]
    g, w, m, v, late_g = take(e), take(e), take(e), take(e), take(l)
    results, late_total = [take(e) for _ in range(3)], refs.pop(0)
    me = lax.axis_index("dp")
    ring = Ring(n, me, shape, EARLY_PIECES, g, w, m, v, results, take(6), take(4))
    held = (*take(2), late_total, None, None, None)
    late = Ring(n, me, late_shape, LATE_PIECES, late_g, None, None, None, (None,) * 3, held, take(4))

    ring.greet()

    @pl.when(odd())
    def _():
        late.first_terms()

    ring.first_terms()

    @pl.when(odd())
    def _():
        late.load_terms()

    ring.load_terms()
    ring.load_states()

    @pl.when(odd())
    def _():
        late.pass_on()
        for p in range(late.pieces):
            late.finish_sum(p)

    ring.pass_on()
    ring.states_loaded()
    for p in range(ring.pieces):
        ring.finish_sum(p)
        ring.step(p)
    ring.gather()
    ring.all_sent(2)
    pl.when(odd())(functools.partial(late.all_sent, 1))


def late_kernel(n, shape, *refs):
    refs = list(refs)
    take = lambda c: [refs.pop(0) for _ in range(c)]
    count = shape[0]
    g, w, m, v, total = take(count), take(count), take(count), take(count), refs.pop(0)
    results = [take(count) for _ in range(3)]
    ring = Ring(n, lax.axis_index("dp"), shape, LATE_PIECES, g, w, m, v, results, take(6), take(4))
    total_sem = refs.pop(0)
    ring.load_states()
    total_copy = pltpu.make_async_copy(total, ring.total, total_sem)
    pl.when(odd())(total_copy.start)
    ring.greet()

    @pl.when(even())
    def _():
        ring.first_terms()
        ring.load_terms()

    pl.when(odd())(total_copy.wait)
    pl.when(even())(ring.pass_on)
    ring.states_loaded()
    pl.when(even())(functools.partial(ring.loaded, 0))
    for p in range(ring.pieces):
        pl.when(even())(functools.partial(ring.finish_sum, p))
        ring.step(p)
    ring.gather()
    pl.when(even())(functools.partial(ring.all_sent, 2))
    pl.when(odd())(functools.partial(ring.all_sent, 1))


def put_kernel(count, *refs):
    sources, results, sem = refs[:count], refs[count:-1], refs[-1]
    copies = [pltpu.make_async_copy(a, b, sem.at[i]) for i, (a, b) in enumerate(zip(sources, results, strict=True))]
    for copy in copies:
        copy.start()
    for copy in copies:
        copy.wait()


def put(arrays):
    count = len(arrays)
    return pl.pallas_call(
        functools.partial(put_kernel, count),
        out_shape=[pltpu.HBM(one.shape, one.dtype) for one in arrays],
        in_specs=[VMEM] * count,
        out_specs=[HBM] * count,
        scratch_shapes=[DMA((count,))],
        compiler_params=pltpu.CompilerParams(vmem_limit_bytes=1 << 20),
    )(*arrays)


def solution(mesh):
    n = mesh.shape["dp"]

    def step(*arrays):
        g, w, m, v = (arrays[i : i + 3] for i in (0, 3, 6, 9))
        early, late = slice(0, 2), slice(2, 3)
        e, l = len(g[early]), len(g[late])
        vmem = lambda several: [pltpu.VMEM(one.shape, one.dtype) for one in several]
        early_shape, late_shape = (e, *m[early][0].shape), (l, *m[late][0].shape)

        *first, total = pl.pallas_call(
            functools.partial(early_kernel, n, early_shape, late_shape),
            out_shape=[*vmem((*w[early], *m[early], *v[early])), pltpu.VMEM((l * late_shape[1], *late_shape[2:]), jnp.bfloat16)],
            in_specs=[HBM] * (4 * e + l),
            out_specs=[VMEM] * (3 * e + 1),
            scratch_shapes=[
                *Ring.scratch(n, EARLY_PIECES, early_shape, True),
                *Ring.scratch(n, LATE_PIECES, late_shape, False),
            ],
            compiler_params=pltpu.CompilerParams(collective_id=0, has_side_effects=True, vmem_limit_bytes=GRANT_EARLY),
        )(*g[early], *w[early], *m[early], *v[early], *g[late])
        *first, total = put([*first, total])
        second = pl.pallas_call(
            functools.partial(late_kernel, n, late_shape),
            out_shape=vmem((*w[late], *m[late], *v[late])),
            in_specs=[HBM] * (4 * l + 1),
            out_specs=[VMEM] * (3 * l),
            scratch_shapes=[*Ring.scratch(n, LATE_PIECES, late_shape, True), DMA],
            compiler_params=pltpu.CompilerParams(collective_id=1, has_side_effects=True, vmem_limit_bytes=GRANT_LATE),
        )(*g[late], *w[late], *m[late], *v[late], total)
        second = put(second)
        return tuple(one for i in range(3) for one in (*first[i * e : (i + 1) * e], *second[i * l : (i + 1) * l]))

    all_of, cut = P(None, None, None), P(None, "dp", None)
    return jax.shard_map(
        step,
        mesh=mesh,
        in_specs=(P(("rep", "dp"), None, None, None),) * 3 + (all_of,) * 3 + (cut,) * 6,
        out_specs=(P("rep", None, None),) * 3 + (P("rep", "dp", None),) * 6,
        check_vma=False,
    )
```

```python
import functools

import jax
import jax.numpy as jnp
from jax import lax
from jax.experimental import pallas as pl
from jax.experimental.pallas import tpu as pltpu
from jax.sharding import PartitionSpec as P

MESH = pl.DeviceIdType.MESH
DMA = pltpu.SemaphoreType.DMA
HBM, VMEM = pl.BlockSpec(memory_space=pltpu.HBM), pl.BlockSpec(memory_space=pltpu.VMEM)
ROWS = 16
EARLY_PIECES, LATE_PIECES = 1, 4
GRANT_EARLY, GRANT_LATE = 54_000_000, 61_500_000


def adamw(w, m, v, g):
    m = 0.9 * m + 0.1 * g
    v = 0.95 * v + 0.05 * g * g
    step = m * lax.rsqrt(v + 1e-8) + 0.1 * w
    return (w - 0.02 * step).astype(jnp.bfloat16), m, v


def by_rows(count, body):
    lax.fori_loop(0, count // ROWS, lambda i, _: body(pl.multiple_of(i * ROWS, ROWS)), None)


class Ring:
    def __init__(self, n, me, shape, pieces, g, w, m, v, results, buffers, sems):
        self.n, self.me, self.g, self.w, self.m, self.v = n, me, g, w, m, v
        self.w_out, self.m_out, self.v_out = results
        self.terms, self.inbox, self.total, self.own, self.m_in, self.v_in = buffers
        self.load_sem, self.state_sem, self.send_sem, self.recv_sem = sems
        self.to = [lax.rem(me + 1, n), lax.rem(me + n - 1, n)]
        weights, self.layers, self.block_rows, _ = shape
        self.parts, self.hops, self.place, self.inbox_rows, self.message, _ = self.cut(n, pieces, shape)
        self.pieces = len(self.parts)
        self.far = n // 2
        self.loads_over = set()

    @staticmethod
    def cut(n, pieces, shape):
        weights, layers, rows, _ = shape
        size = -(-rows // (pieces * ROWS)) * ROWS
        parts, hops, place, message = [], [], {}, {}
        end = [0, 0]
        for k in range(weights):
            for layer in range(layers):
                for i, r in enumerate(range(0, rows, size)):
                    p, count = len(parts), min(size, rows - r)
                    parts.append((k, layer, r, count))
                    ways = (n // 2, (n - 1) // 2)
                    hops.append(ways if (i + layer) % 2 == 0 else ways[::-1])
                    for s in (0, 1):
                        for left in range(1, hops[p][s] + 1):
                            place[p, s, left] = end[s]
                            end[s] += count
                            message[p, s, left] = len(message)
        assert end[0] == end[1]
        return parts, hops, place, end[0], message, len(message)

    @classmethod
    def scratch(cls, n, pieces, shape):
        weights, layers, rows, columns = shape
        _, _, _, inbox_rows, _, messages = cls.cut(n, pieces, shape)
        whole = (weights * layers, rows, columns)
        data = [pltpu.VMEM((n, *whole), jnp.bfloat16), pltpu.VMEM((2 * inbox_rows, columns), jnp.bfloat16)]
        data += [pltpu.VMEM(whole, t) for t in (jnp.bfloat16, jnp.bfloat16, jnp.float32, jnp.float32)]
        return [*data, DMA((n,)), DMA((3,)), DMA((2,)), DMA((messages,))]

    def at(self, away):
        return lax.rem(self.me + (away + self.n), self.n)

    def block(self, owner):
        return pl.ds(pl.multiple_of(owner * self.block_rows, self.block_rows), self.block_rows)

    def rows(self, p, owner):
        _, _, first, count = self.parts[p]
        return pl.ds(pl.multiple_of(owner * self.block_rows + first, ROWS), count)

    def matrix(self, p):
        k, layer, *_ = self.parts[p]
        return k * self.layers + layer

    def term(self, p, away):
        _, _, first, count = self.parts[p]
        return self.terms.at[away % self.n, self.matrix(p), pl.ds(first, count)]

    def came(self, p, side, left):
        return self.inbox.at[pl.ds(side * self.inbox_rows + self.place[p, side, left], self.parts[p][3])]

    def load_terms(self):
        for left in range(self.far - 1, -1, -1):
            for away in sorted({left, -left}):
                for k, g in enumerate(self.g):
                    target = self.terms.at[away % self.n, pl.ds(k * self.layers, self.layers)]
                    pltpu.make_async_copy(g.at[0, :, self.block(self.at(away))], target, self.load_sem.at[away % self.n]).start()

    def loaded(self, away):
        if away not in self.loads_over:
            self.loads_over.add(away)
            whole = self.terms.at[away % self.n]
            pltpu.make_async_copy(whole, whole, self.load_sem.at[away % self.n]).wait()

    def load_states(self):
        for k in range(len(self.g)):
            mine = pl.ds(k * self.layers, self.layers)
            sources = (self.w[k].at[:, self.block(self.me)], self.m[k], self.v[k])
            for i, (source, target) in enumerate(zip(sources, (self.own, self.m_in, self.v_in), strict=True)):
                pltpu.make_async_copy(source, target.at[mine], self.state_sem.at[i]).start()

    def states_loaded(self):
        for i, whole in enumerate((self.own, self.m_in, self.v_in)):
            pltpu.make_async_copy(whole, whole, self.state_sem.at[i]).wait()

    def remote(self, side, source, target, recv_sem):
        return pltpu.make_async_remote_copy(
            src_ref=source,
            dst_ref=target,
            send_sem=self.send_sem.at[side],
            recv_sem=self.recv_sem.at[recv_sem],
            device_id={"dp": self.to[side]},
            device_id_type=MESH,
        )

    def sum_copy(self, p, side, left):
        away = left if side == 0 else -left
        if self.hops[p][side] == left:
            k, layer, *_ = self.parts[p]
            source = self.g[k].at[0, layer, self.rows(p, self.at(away))]
        else:
            source = self.term(p, away)
        return self.remote(side, source, self.came(p, side, left), self.message[p, side, left])

    def gather_copy(self, p, side, hop, back, done=None):
        away = hop - back
        k, layer, *_ = self.parts[p]
        block = (layer, self.rows(p, self.at(-away if side == 0 else away)))
        return self.remote(side, (done or self.w_out)[k].at[block], self.w_out[k].at[block], self.message[p, side, self.hops[p][side] + 1 - hop])

    def live(self, side, hops):
        return [p for p in range(self.pieces) if self.hops[p][side] >= hops]

    def first_terms(self):
        for left in range(self.far, 0, -1):
            for order in zip(*([p for p in range(self.pieces) if self.hops[p][s] == left] for s in (0, 1)), strict=True):
                for s, p in enumerate(order):
                    self.sum_copy(p, s, left).start()

    def pass_on(self):
        for left in range(self.far - 1, 0, -1):
            for order in zip(*(self.live(s, left + 1) for s in (0, 1)), strict=True):
                for s, p in enumerate(order):
                    away = left if s == 0 else -left
                    self.loaded(away)
                    self.sum_copy(p, s, left + 1).wait_recv()
                    here, came = self.term(p, away), self.came(p, s, left + 1)

                    def add(r, here=here, came=came):
                        r = pl.ds(r, ROWS)
                        here[r, :] = (here[r, :].astype(jnp.float32) + came[r, :].astype(jnp.float32)).astype(jnp.bfloat16)

                    by_rows(self.parts[p][3], add)
                    self.sum_copy(p, s, left).start()

    def finish_sum(self, p):
        for s in (0, 1):
            self.sum_copy(p, s, 1).wait_recv()
        _, _, first, count = self.parts[p]

        def add(r):
            here = pl.ds(r, ROWS)
            parts = [ref[here, :].astype(jnp.float32) for ref in (self.term(p, 0), self.came(p, 0, 1), self.came(p, 1, 1))]
            self.total.at[self.matrix(p)][pl.ds(first + r, ROWS), :] = (parts[0] + parts[1] + parts[2]).astype(jnp.bfloat16)

        by_rows(count, add)

    def step(self, p):
        k, layer, first, count = self.parts[p]

        def take(r):
            rows = pl.ds(first + r, ROWS)
            w, m, v, g = (ref.at[self.matrix(p)][rows, :] for ref in (self.own, self.m_in, self.v_in, self.total))
            new = adamw(w.astype(jnp.float32), m, v, g.astype(jnp.float32))
            self.w_out[k].at[layer][pl.ds(pl.multiple_of(self.me * self.block_rows + (first + r), ROWS), ROWS), :] = new[0]
            self.m_out[k].at[layer][rows, :] = new[1]
            self.v_out[k].at[layer][rows, :] = new[2]

        by_rows(count, take)
        for s in (0, 1):
            self.gather_copy(p, s, 1, 1).start()

    def take_steps(self):
        self.loaded(0)
        self.states_loaded()
        for p in range(self.pieces):
            self.finish_sum(p)
            self.step(p)

    def spread(self, hop, done=None):
        order = [self.live(s, hop) for s in (0, 1)]
        for s in (0, 1):
            if hop == self.far - 1:
                order[s].sort(key=lambda p, s=s: -self.hops[p][s])
        for pair in zip(*order, strict=True):
            for s, p in enumerate(pair):
                if done is None:
                    self.gather_copy(p, s, hop - 1, 0).wait_recv()
                self.gather_copy(p, s, hop, 1, done).start()

    def gathered(self, hops):
        for hop in range(1, hops + 1):
            for p in range(self.pieces):
                for s in (0, 1):
                    if min(self.hops[p][s], hops) == hop:
                        self.gather_copy(p, s, hop, 0).wait_recv()

    def all_sent(self, hops, sums):
        for s in (0, 1):
            rows = sum(self.parts[p][3] for hop in hops for p in self.live(s, hop)) + sums * self.inbox_rows
            whole = self.inbox.at[pl.ds(0, rows)]
            pltpu.make_async_copy(whole, whole, self.send_sem.at[s]).wait()

    def greet(self):
        barrier = pltpu.get_barrier_semaphore()
        for neighbour in self.to:
            pl.semaphore_signal(barrier, inc=1, device_id={"dp": neighbour}, device_id_type=MESH)
        pl.semaphore_wait(barrier, 2)


def ahead():
    return lax.rem(lax.axis_index("rep"), 2) == 0


def behind():
    return lax.rem(lax.axis_index("rep"), 2) == 1


def early_hops(n):
    return n // 2 - 2


def early_kernel(n, shape, late_shape, *refs):
    refs = list(refs)
    take = lambda c: [refs.pop(0) for _ in range(c)]
    e, l = shape[0], late_shape[0]
    data, late_data = [take(e) for _ in range(4)], [take(l) for _ in range(4)]
    results, late_results = [take(e) for _ in range(3)], [take(l) for _ in range(3)]
    me = lax.axis_index("dp")
    ring = Ring(n, me, shape, EARLY_PIECES, *data, results, take(6), take(4))
    late = Ring(n, me, late_shape, LATE_PIECES, *late_data, late_results, take(6), take(4))

    ring.greet()
    pl.when(ahead())(late.first_terms)
    ring.first_terms()

    @pl.when(ahead())
    def _():
        late.load_terms()
        late.load_states()

    ring.load_terms()
    ring.load_states()

    @pl.when(ahead())
    def _():
        late.pass_on()
        late.take_steps()

    ring.pass_on()
    ring.take_steps()
    for hop in range(2, ring.far + 1):
        if hop <= early_hops(n):
            pl.when(ahead())(functools.partial(late.spread, hop))
        ring.spread(hop)
    ring.gathered(ring.far)
    ring.all_sent(range(1, ring.far + 1), True)

    @pl.when(ahead())
    def _():
        late.gathered(early_hops(n))
        late.all_sent(range(1, early_hops(n) + 1), True)


def late_kernel(n, shape, *refs):
    refs = list(refs)
    take = lambda c: [refs.pop(0) for _ in range(c)]
    count = shape[0]
    data, done = [take(count) for _ in range(4)], take(count)
    results = [take(count) for _ in range(3)]
    ring = Ring(n, lax.axis_index("dp"), shape, LATE_PIECES, *data, results, take(6), take(4))
    last = range(early_hops(n) + 1, ring.far + 1)
    ring.greet()

    @pl.when(ahead())
    def _():
        ring.spread(last[0], done)

    @pl.when(behind())
    def _():
        ring.first_terms()
        ring.load_terms()
        ring.load_states()
        ring.pass_on()
        ring.take_steps()
        for hop in range(2, last[0] + 1):
            ring.spread(hop)

    for hop in last[1:]:
        ring.spread(hop)
    ring.gathered(ring.far)
    pl.when(ahead())(functools.partial(ring.all_sent, last, False))
    pl.when(behind())(functools.partial(ring.all_sent, range(1, ring.far + 1), True))


def put_early_kernel(n, e, l, *refs):
    refs, sem = list(refs[:-1]), refs[-1]
    count = 3 * (e + l)
    sources, results = refs[:count], refs[count:]
    early = [pltpu.make_async_copy(sources[i], results[i], sem.at[i]) for i in range(3 * e)]
    for copy in early:
        copy.start()

    @pl.when(ahead())
    def _():
        reach = early_hops(n)
        late = [pltpu.make_async_copy(sources[i], results[i], sem.at[i]) for i in range(3 * e + l, count)]
        late += block_copies(n, sources[3 * e : 3 * e + l], results[3 * e : 3 * e + l], range(-reach, reach + 1), sem, count)
        for copy in late:
            copy.start()
        for copy in late:
            copy.wait()

    for copy in early:
        copy.wait()


def block_copies(n, sources, results, aways, sem, first):
    me = lax.axis_index("dp")
    copies = []
    for source, result in zip(sources, results, strict=True):
        rows = source.shape[1] // n
        for away in aways:
            block = pl.ds(pl.multiple_of(lax.rem(me + (away + n), n) * rows, rows), rows)
            copies.append(pltpu.make_async_copy(source.at[:, block], result.at[:, block], sem.at[first + len(copies)]))
    return copies


def put_late_kernel(n, l, *refs):
    sources, results, sem = refs[: 3 * l], refs[6 * l : 9 * l], refs[-1]

    @pl.when(ahead())
    def _():
        reach = early_hops(n)
        copies = block_copies(n, sources[:l], results[:l], range(reach + 1, n - reach), sem, 3 * l)
        for copy in copies:
            copy.start()
        for copy in copies:
            copy.wait()

    @pl.when(behind())
    def _():
        copies = [pltpu.make_async_copy(sources[i], results[i], sem.at[i]) for i in range(3 * l)]
        for copy in copies:
            copy.start()
        for copy in copies:
            copy.wait()


def solution(mesh):
    n = mesh.shape["dp"]

    def step(*arrays):
        g, w, m, v = (arrays[i : i + 3] for i in (0, 3, 6, 9))
        early, late = slice(0, 2), slice(2, 3)
        e, l = len(g[early]), len(g[late])
        vmem = lambda several: [pltpu.VMEM(one.shape, one.dtype) for one in several]
        hbm = lambda several: [pltpu.HBM(one.shape, one.dtype) for one in several]
        early_shape, late_shape = (e, *m[early][0].shape), (l, *m[late][0].shape)
        early_results, late_results = (*w[early], *m[early], *v[early]), (*w[late], *m[late], *v[late])

        first = pl.pallas_call(
            functools.partial(early_kernel, n, early_shape, late_shape),
            out_shape=vmem((*early_results, *late_results)),
            in_specs=[HBM] * (4 * (e + l)),
            out_specs=[VMEM] * (3 * (e + l)),
            scratch_shapes=[*Ring.scratch(n, EARLY_PIECES, early_shape), *Ring.scratch(n, LATE_PIECES, late_shape)],
            compiler_params=pltpu.CompilerParams(collective_id=0, has_side_effects=True, vmem_limit_bytes=GRANT_EARLY),
        )(*g[early], *w[early], *m[early], *v[early], *g[late], *w[late], *m[late], *v[late])
        first = pl.pallas_call(
            functools.partial(put_early_kernel, n, e, l),
            out_shape=hbm((*early_results, *late_results)),
            in_specs=[VMEM] * (3 * (e + l)),
            out_specs=[HBM] * (3 * (e + l)),
            scratch_shapes=[DMA((3 * (e + l) + l * (2 * early_hops(n) + 1),))],
            compiler_params=pltpu.CompilerParams(vmem_limit_bytes=1 << 20),
        )(*first)
        first, half = first[: 3 * e], first[3 * e :]
        second = pl.pallas_call(
            functools.partial(late_kernel, n, late_shape),
            out_shape=vmem(late_results),
            in_specs=[HBM] * (5 * l),
            out_specs=[VMEM] * (3 * l),
            scratch_shapes=Ring.scratch(n, LATE_PIECES, late_shape),
            compiler_params=pltpu.CompilerParams(collective_id=1, has_side_effects=True, vmem_limit_bytes=GRANT_LATE),
        )(*g[late], *w[late], *m[late], *v[late], *half[:l])
        second = pl.pallas_call(
            functools.partial(put_late_kernel, n, l),
            out_shape=hbm(late_results),
            in_specs=[VMEM] * (3 * l) + [HBM] * (3 * l),
            out_specs=[HBM] * (3 * l),
            scratch_shapes=[DMA((3 * l + l * (n - 1 - 2 * early_hops(n)),))],
            input_output_aliases={3 * l + i: i for i in range(3 * l)},
            compiler_params=pltpu.CompilerParams(vmem_limit_bytes=1 << 20),
        )(*second, *half)
        return tuple(one for i in range(3) for one in (*first[i * e : (i + 1) * e], *second[i * l : (i + 1) * l]))

    all_of, cut = P(None, None, None), P(None, "dp", None)
    return jax.shard_map(
        step,
        mesh=mesh,
        in_specs=(P(("rep", "dp"), None, None, None),) * 3 + (all_of,) * 3 + (cut,) * 6,
        out_specs=(P("rep", None, None),) * 3 + (P("rep", "dp", None),) * 6,
        check_vma=False,
    )
```

```python
import functools

import jax
import jax.numpy as jnp
from jax import lax
from jax.experimental import pallas as pl
from jax.experimental.pallas import tpu as pltpu
from jax.sharding import PartitionSpec as P

MESH = pl.DeviceIdType.MESH
DMA = pltpu.SemaphoreType.DMA
HBM, VMEM = pl.BlockSpec(memory_space=pltpu.HBM), pl.BlockSpec(memory_space=pltpu.VMEM)
ROWS = 16
EARLY_PIECES, LATE_PIECES = 1, 4
HOLD = 2400
GRANT_EARLY, GRANT_LATE = 54_000_000, 61_500_000


def adamw(w, m, v, g):
    m = 0.9 * m + 0.1 * g
    v = 0.95 * v + 0.05 * g * g
    step = m * lax.rsqrt(v + 1e-8) + 0.1 * w
    return (w - 0.02 * step).astype(jnp.bfloat16), m, v


def by_rows(count, body):
    lax.fori_loop(0, count // ROWS, lambda i, _: body(pl.multiple_of(i * ROWS, ROWS)), None)


class Ring:
    def __init__(self, n, me, shape, pieces, g, w, m, v, results, buffers, sems):
        self.n, self.me, self.g, self.w, self.m, self.v = n, me, g, w, m, v
        self.w_out, self.m_out, self.v_out = results
        self.terms, self.inbox, self.total, self.own, self.m_in, self.v_in = buffers
        self.load_sem, self.state_sem, self.send_sem, self.recv_sem = sems
        self.to = [lax.rem(me + 1, n), lax.rem(me + n - 1, n)]
        weights, self.layers, self.block_rows, _ = shape
        self.parts, self.hops, self.place, self.inbox_rows, self.message, _ = self.cut(n, pieces, shape)
        self.pieces = len(self.parts)
        self.far = n // 2
        self.loads_over = set()

    @staticmethod
    def cut(n, pieces, shape):
        weights, layers, rows, _ = shape
        size = -(-rows // (pieces * ROWS)) * ROWS
        parts, hops, place, message = [], [], {}, {}
        end = [0, 0]
        for k in range(weights):
            for layer in range(layers):
                for i, r in enumerate(range(0, rows, size)):
                    p, count = len(parts), min(size, rows - r)
                    parts.append((k, layer, r, count))
                    ways = (n // 2, (n - 1) // 2)
                    hops.append(ways if (i + layer) % 2 == 0 else ways[::-1])
                    for s in (0, 1):
                        for left in range(1, hops[p][s] + 1):
                            place[p, s, left] = end[s]
                            end[s] += count
                            message[p, s, left] = len(message)
        assert end[0] == end[1]
        return parts, hops, place, end[0], message, len(message)

    @classmethod
    def scratch(cls, n, pieces, shape):
        weights, layers, rows, columns = shape
        _, _, _, inbox_rows, _, messages = cls.cut(n, pieces, shape)
        whole = (weights * layers, rows, columns)
        data = [pltpu.VMEM((n, *whole), jnp.bfloat16), pltpu.VMEM((2 * inbox_rows, columns), jnp.bfloat16)]
        data += [pltpu.VMEM(whole, t) for t in (jnp.bfloat16, jnp.bfloat16, jnp.float32, jnp.float32)]
        return [*data, DMA((n,)), DMA((3,)), DMA((2,)), DMA((messages,))]

    def at(self, away):
        return lax.rem(self.me + (away + self.n), self.n)

    def block(self, owner):
        return pl.ds(pl.multiple_of(owner * self.block_rows, self.block_rows), self.block_rows)

    def rows(self, p, owner):
        _, _, first, count = self.parts[p]
        return pl.ds(pl.multiple_of(owner * self.block_rows + first, ROWS), count)

    def matrix(self, p):
        k, layer, *_ = self.parts[p]
        return k * self.layers + layer

    def term(self, p, away):
        _, _, first, count = self.parts[p]
        return self.terms.at[away % self.n, self.matrix(p), pl.ds(first, count)]

    def came(self, p, side, left):
        return self.inbox.at[pl.ds(side * self.inbox_rows + self.place[p, side, left], self.parts[p][3])]

    def load_terms(self):
        for left in range(self.far - 1, -1, -1):
            for away in sorted({left, -left}):
                for k, g in enumerate(self.g):
                    target = self.terms.at[away % self.n, pl.ds(k * self.layers, self.layers)]
                    pltpu.make_async_copy(g.at[0, :, self.block(self.at(away))], target, self.load_sem.at[away % self.n]).start()

    def loaded(self, away):
        if away not in self.loads_over:
            self.loads_over.add(away)
            whole = self.terms.at[away % self.n]
            pltpu.make_async_copy(whole, whole, self.load_sem.at[away % self.n]).wait()

    def load_states(self):
        for k in range(len(self.g)):
            mine = pl.ds(k * self.layers, self.layers)
            sources = (self.w[k].at[:, self.block(self.me)], self.m[k], self.v[k])
            for i, (source, target) in enumerate(zip(sources, (self.own, self.m_in, self.v_in), strict=True)):
                pltpu.make_async_copy(source, target.at[mine], self.state_sem.at[i]).start()

    def states_loaded(self):
        for i, whole in enumerate((self.own, self.m_in, self.v_in)):
            pltpu.make_async_copy(whole, whole, self.state_sem.at[i]).wait()

    def remote(self, side, source, target, recv_sem):
        return pltpu.make_async_remote_copy(
            src_ref=source,
            dst_ref=target,
            send_sem=self.send_sem.at[side],
            recv_sem=self.recv_sem.at[recv_sem],
            device_id={"dp": self.to[side]},
            device_id_type=MESH,
        )

    def sum_copy(self, p, side, left):
        away = left if side == 0 else -left
        if self.hops[p][side] == left:
            k, layer, *_ = self.parts[p]
            source = self.g[k].at[0, layer, self.rows(p, self.at(away))]
        else:
            source = self.term(p, away)
        return self.remote(side, source, self.came(p, side, left), self.message[p, side, left])

    def gather_copy(self, p, side, hop, back, done=None):
        away = hop - back
        k, layer, *_ = self.parts[p]
        block = (layer, self.rows(p, self.at(-away if side == 0 else away)))
        return self.remote(side, (done or self.w_out)[k].at[block], self.w_out[k].at[block], self.message[p, side, self.hops[p][side] + 1 - hop])

    def live(self, side, hops):
        return [p for p in range(self.pieces) if self.hops[p][side] >= hops]

    def first_terms(self):
        for left in range(self.far, 0, -1):
            for order in zip(*([p for p in range(self.pieces) if self.hops[p][s] == left] for s in (0, 1)), strict=True):
                for s, p in enumerate(order):
                    self.sum_copy(p, s, left).start()

    def pass_on(self):
        for left in range(self.far - 1, 0, -1):
            for order in zip(*(self.live(s, left + 1) for s in (0, 1)), strict=True):
                for s, p in enumerate(order):
                    away = left if s == 0 else -left
                    self.loaded(away)
                    self.sum_copy(p, s, left + 1).wait_recv()
                    here, came = self.term(p, away), self.came(p, s, left + 1)

                    def add(r, here=here, came=came):
                        r = pl.ds(r, ROWS)
                        here[r, :] = (here[r, :].astype(jnp.float32) + came[r, :].astype(jnp.float32)).astype(jnp.bfloat16)

                    by_rows(self.parts[p][3], add)
                    self.sum_copy(p, s, left).start()

    def finish_sum(self, p):
        for s in (0, 1):
            self.sum_copy(p, s, 1).wait_recv()
        _, _, first, count = self.parts[p]

        def add(r):
            here = pl.ds(r, ROWS)
            parts = [ref[here, :].astype(jnp.float32) for ref in (self.term(p, 0), self.came(p, 0, 1), self.came(p, 1, 1))]
            self.total.at[self.matrix(p)][pl.ds(first + r, ROWS), :] = (parts[0] + parts[1] + parts[2]).astype(jnp.bfloat16)

        by_rows(count, add)

    def step(self, p):
        k, layer, first, count = self.parts[p]

        def take(r):
            rows = pl.ds(first + r, ROWS)
            w, m, v, g = (ref.at[self.matrix(p)][rows, :] for ref in (self.own, self.m_in, self.v_in, self.total))
            new = adamw(w.astype(jnp.float32), m, v, g.astype(jnp.float32))
            self.w_out[k].at[layer][pl.ds(pl.multiple_of(self.me * self.block_rows + (first + r), ROWS), ROWS), :] = new[0]
            self.m_out[k].at[layer][rows, :] = new[1]
            self.v_out[k].at[layer][rows, :] = new[2]

        by_rows(count, take)
        for s in (0, 1):
            self.gather_copy(p, s, 1, 1).start()

    def take_steps(self):
        self.loaded(0)
        self.states_loaded()
        for p in range(self.pieces):
            self.finish_sum(p)
            self.step(p)

    def spread(self, hop, done=None):
        order = [self.live(s, hop) for s in (0, 1)]
        for s in (0, 1):
            if hop == self.far - 1:
                order[s].sort(key=lambda p, s=s: -self.hops[p][s])
        for pair in zip(*order, strict=True):
            for s, p in enumerate(pair):
                if done is None:
                    self.gather_copy(p, s, hop - 1, 0).wait_recv()
                self.gather_copy(p, s, hop, 1, done).start()

    def gathered(self, hops):
        for hop in range(1, hops + 1):
            for p in range(self.pieces):
                for s in (0, 1):
                    if min(self.hops[p][s], hops) == hop:
                        self.gather_copy(p, s, hop, 0).wait_recv()

    def all_sent(self, hops, sums):
        for s in (0, 1):
            rows = sum(self.parts[p][3] for hop in hops for p in self.live(s, hop)) + sums * self.inbox_rows
            whole = self.inbox.at[pl.ds(0, rows)]
            pltpu.make_async_copy(whole, whole, self.send_sem.at[s]).wait()

    def greet(self):
        barrier = pltpu.get_barrier_semaphore()
        for neighbour in self.to:
            pl.semaphore_signal(barrier, inc=1, device_id={"dp": neighbour}, device_id_type=MESH)
        pl.semaphore_wait(barrier, 2)


def ahead():
    return lax.rem(lax.axis_index("rep"), 2) == 0


def behind():
    return lax.rem(lax.axis_index("rep"), 2) == 1


def early_hops(n):
    return n // 2 - 2


def early_kernel(n, shape, late_shape, *refs):
    refs = list(refs)
    take = lambda c: [refs.pop(0) for _ in range(c)]
    e, l = shape[0], late_shape[0]
    data, late_data = [take(e) for _ in range(4)], [take(l) for _ in range(4)]
    results, late_results = [take(e) for _ in range(3)], [take(l) for _ in range(3)]
    me = lax.axis_index("dp")
    ring = Ring(n, me, shape, EARLY_PIECES, *data, results, take(6), take(4))
    late = Ring(n, me, late_shape, LATE_PIECES, *late_data, late_results, take(6), take(4))

    ring.greet()
    pl.when(ahead())(late.first_terms)
    ring.first_terms()

    @pl.when(ahead())
    def _():
        late.load_terms()
        late.load_states()

    ring.load_terms()
    ring.load_states()

    @pl.when(ahead())
    def _():
        late.pass_on()
        late.take_steps()

    ring.pass_on()
    ring.take_steps()
    for hop in range(2, ring.far + 1):
        if hop <= early_hops(n):
            pl.when(ahead())(functools.partial(late.spread, hop))
        ring.spread(hop)
    ring.gathered(ring.far)
    ring.all_sent(range(1, ring.far + 1), True)

    @pl.when(ahead())
    def _():
        late.gathered(early_hops(n))
        late.all_sent(range(1, early_hops(n) + 1), True)


def late_kernel(n, shape, *refs):
    refs = list(refs)
    take = lambda c: [refs.pop(0) for _ in range(c)]
    count = shape[0]
    data, done = [take(count) for _ in range(4)], take(count)
    results = [take(count) for _ in range(3)]
    ring = Ring(n, lax.axis_index("dp"), shape, LATE_PIECES, *data, results, take(6), take(4))
    last = range(early_hops(n) + 1, ring.far + 1)
    ring.greet()

    @pl.when(ahead())
    def _():
        pl.delay(HOLD)
        ring.spread(last[0], done)

    @pl.when(behind())
    def _():
        ring.first_terms()
        ring.load_terms()
        ring.load_states()
        ring.pass_on()
        ring.take_steps()
        for hop in range(2, last[0] + 1):
            ring.spread(hop)

    for hop in last[1:]:
        ring.spread(hop)
    ring.gathered(ring.far)
    pl.when(ahead())(functools.partial(ring.all_sent, last, False))
    pl.when(behind())(functools.partial(ring.all_sent, range(1, ring.far + 1), True))


def put_early_kernel(n, e, l, *refs):
    refs, sem = list(refs[:-1]), refs[-1]
    count = 3 * (e + l)
    sources, results = refs[:count], refs[count:]
    early = [pltpu.make_async_copy(sources[i], results[i], sem.at[i]) for i in range(3 * e)]
    for copy in early:
        copy.start()

    @pl.when(ahead())
    def _():
        reach = early_hops(n)
        late = [pltpu.make_async_copy(sources[i], results[i], sem.at[i]) for i in range(3 * e + l, count)]
        late += block_copies(n, sources[3 * e : 3 * e + l], results[3 * e : 3 * e + l], range(-reach, reach + 1), sem, count)
        for copy in late:
            copy.start()
        for copy in late:
            copy.wait()

    for copy in early:
        copy.wait()


def block_copies(n, sources, results, aways, sem, first):
    me = lax.axis_index("dp")
    copies = []
    for source, result in zip(sources, results, strict=True):
        rows = source.shape[1] // n
        for away in aways:
            block = pl.ds(pl.multiple_of(lax.rem(me + (away + n), n) * rows, rows), rows)
            copies.append(pltpu.make_async_copy(source.at[:, block], result.at[:, block], sem.at[first + len(copies)]))
    return copies


def put_late_kernel(n, l, *refs):
    sources, results, sem = refs[: 3 * l], refs[6 * l : 9 * l], refs[-1]

    @pl.when(ahead())
    def _():
        reach = early_hops(n)
        copies = block_copies(n, sources[:l], results[:l], range(reach + 1, n - reach), sem, 3 * l)
        for copy in copies:
            copy.start()
        for copy in copies:
            copy.wait()

    @pl.when(behind())
    def _():
        copies = [pltpu.make_async_copy(sources[i], results[i], sem.at[i]) for i in range(3 * l)]
        for copy in copies:
            copy.start()
        for copy in copies:
            copy.wait()


def solution(mesh):
    n = mesh.shape["dp"]

    def step(*arrays):
        g, w, m, v = (arrays[i : i + 3] for i in (0, 3, 6, 9))
        early, late = slice(0, 2), slice(2, 3)
        e, l = len(g[early]), len(g[late])
        vmem = lambda several: [pltpu.VMEM(one.shape, one.dtype) for one in several]
        hbm = lambda several: [pltpu.HBM(one.shape, one.dtype) for one in several]
        early_shape, late_shape = (e, *m[early][0].shape), (l, *m[late][0].shape)
        early_results, late_results = (*w[early], *m[early], *v[early]), (*w[late], *m[late], *v[late])

        first = pl.pallas_call(
            functools.partial(early_kernel, n, early_shape, late_shape),
            out_shape=vmem((*early_results, *late_results)),
            in_specs=[HBM] * (4 * (e + l)),
            out_specs=[VMEM] * (3 * (e + l)),
            scratch_shapes=[*Ring.scratch(n, EARLY_PIECES, early_shape), *Ring.scratch(n, LATE_PIECES, late_shape)],
            compiler_params=pltpu.CompilerParams(collective_id=0, has_side_effects=True, vmem_limit_bytes=GRANT_EARLY),
        )(*g[early], *w[early], *m[early], *v[early], *g[late], *w[late], *m[late], *v[late])
        first = pl.pallas_call(
            functools.partial(put_early_kernel, n, e, l),
            out_shape=hbm((*early_results, *late_results)),
            in_specs=[VMEM] * (3 * (e + l)),
            out_specs=[HBM] * (3 * (e + l)),
            scratch_shapes=[DMA((3 * (e + l) + l * (2 * early_hops(n) + 1),))],
            compiler_params=pltpu.CompilerParams(vmem_limit_bytes=1 << 20),
        )(*first)
        first, half = first[: 3 * e], first[3 * e :]
        second = pl.pallas_call(
            functools.partial(late_kernel, n, late_shape),
            out_shape=vmem(late_results),
            in_specs=[HBM] * (5 * l),
            out_specs=[VMEM] * (3 * l),
            scratch_shapes=Ring.scratch(n, LATE_PIECES, late_shape),
            compiler_params=pltpu.CompilerParams(collective_id=1, has_side_effects=True, vmem_limit_bytes=GRANT_LATE),
        )(*g[late], *w[late], *m[late], *v[late], *half[:l])
        second = pl.pallas_call(
            functools.partial(put_late_kernel, n, l),
            out_shape=hbm(late_results),
            in_specs=[VMEM] * (3 * l) + [HBM] * (3 * l),
            out_specs=[HBM] * (3 * l),
            scratch_shapes=[DMA((3 * l + l * (n - 1 - 2 * early_hops(n)),))],
            input_output_aliases={3 * l + i: i for i in range(3 * l)},
            compiler_params=pltpu.CompilerParams(vmem_limit_bytes=1 << 20),
        )(*second, *half)
        return tuple(one for i in range(3) for one in (*first[i * e : (i + 1) * e], *second[i * l : (i + 1) * l]))

    all_of, cut = P(None, None, None), P(None, "dp", None)
    return jax.shard_map(
        step,
        mesh=mesh,
        in_specs=(P(("rep", "dp"), None, None, None),) * 3 + (all_of,) * 3 + (cut,) * 6,
        out_specs=(P("rep", None, None),) * 3 + (P("rep", "dp", None),) * 6,
        check_vma=False,
    )
```

```python
import functools

import jax
import jax.numpy as jnp
from jax import lax
from jax.experimental import pallas as pl
from jax.experimental.pallas import tpu as pltpu
from jax.sharding import PartitionSpec as P

MESH = pl.DeviceIdType.MESH
DMA = pltpu.SemaphoreType.DMA
HBM, VMEM = pl.BlockSpec(memory_space=pltpu.HBM), pl.BlockSpec(memory_space=pltpu.VMEM)
ROWS = 16
EARLY_PIECES, LATE_PIECES = 1, 2
HOLD = 3200
GRANT_EARLY, GRANT_LATE = 54_000_000, 61_500_000


def adamw(w, m, v, g):
    m = 0.9 * m + 0.1 * g
    v = 0.95 * v + 0.05 * g * g
    step = m * lax.rsqrt(v + 1e-8) + 0.1 * w
    return (w - 0.02 * step).astype(jnp.bfloat16), m, v


def by_rows(count, body):
    lax.fori_loop(0, count // ROWS, lambda i, _: body(pl.multiple_of(i * ROWS, ROWS)), None)


class Ring:
    def __init__(self, n, me, shape, pieces, g, w, m, v, results, buffers, sems):
        self.n, self.me, self.g, self.w, self.m, self.v = n, me, g, w, m, v
        self.w_out, self.m_out, self.v_out = results
        self.terms, self.inbox, self.total, self.own, self.m_in, self.v_in = buffers
        self.load_sem, self.state_sem, self.send_sem, self.recv_sem = sems
        self.to = [lax.rem(me + 1, n), lax.rem(me + n - 1, n)]
        weights, self.layers, self.block_rows, _ = shape
        self.parts, self.hops, self.place, self.inbox_rows, self.message, _ = self.cut(n, pieces, shape)
        self.pieces = len(self.parts)
        self.far = n // 2
        self.loads_over = set()

    @staticmethod
    def cut(n, pieces, shape):
        weights, layers, rows, _ = shape
        size = -(-rows // (pieces * ROWS)) * ROWS
        parts, hops, place, message = [], [], {}, {}
        end = [0, 0]
        for k in range(weights):
            for layer in range(layers):
                for i, r in enumerate(range(0, rows, size)):
                    p, count = len(parts), min(size, rows - r)
                    parts.append((k, layer, r, count))
                    ways = (n // 2, (n - 1) // 2)
                    hops.append(ways if (i + layer) % 2 == 0 else ways[::-1])
                    for s in (0, 1):
                        for left in range(1, hops[p][s] + 1):
                            place[p, s, left] = end[s]
                            end[s] += count
                            message[p, s, left] = len(message)
        assert end[0] == end[1]
        return parts, hops, place, end[0], message, len(message)

    @classmethod
    def scratch(cls, n, pieces, shape):
        weights, layers, rows, columns = shape
        _, _, _, inbox_rows, _, messages = cls.cut(n, pieces, shape)
        whole = (weights * layers, rows, columns)
        data = [pltpu.VMEM((n, *whole), jnp.bfloat16), pltpu.VMEM((2 * inbox_rows, columns), jnp.bfloat16)]
        data += [pltpu.VMEM(whole, t) for t in (jnp.bfloat16, jnp.bfloat16, jnp.float32, jnp.float32)]
        return [*data, DMA((n,)), DMA((3,)), DMA((2,)), DMA((messages,))]

    def at(self, away):
        return lax.rem(self.me + (away + self.n), self.n)

    def block(self, owner):
        return pl.ds(pl.multiple_of(owner * self.block_rows, self.block_rows), self.block_rows)

    def rows(self, p, owner):
        _, _, first, count = self.parts[p]
        return pl.ds(pl.multiple_of(owner * self.block_rows + first, ROWS), count)

    def matrix(self, p):
        k, layer, *_ = self.parts[p]
        return k * self.layers + layer

    def term(self, p, away):
        _, _, first, count = self.parts[p]
        return self.terms.at[away % self.n, self.matrix(p), pl.ds(first, count)]

    def came(self, p, side, left):
        return self.inbox.at[pl.ds(side * self.inbox_rows + self.place[p, side, left], self.parts[p][3])]

    def load_terms(self):
        for left in range(self.far - 1, -1, -1):
            for away in sorted({left, -left}):
                for k, g in enumerate(self.g):
                    target = self.terms.at[away % self.n, pl.ds(k * self.layers, self.layers)]
                    pltpu.make_async_copy(g.at[0, :, self.block(self.at(away))], target, self.load_sem.at[away % self.n]).start()

    def loaded(self, away):
        if away not in self.loads_over:
            self.loads_over.add(away)
            whole = self.terms.at[away % self.n]
            pltpu.make_async_copy(whole, whole, self.load_sem.at[away % self.n]).wait()

    def load_states(self):
        for k in range(len(self.g)):
            mine = pl.ds(k * self.layers, self.layers)
            sources = (self.w[k].at[:, self.block(self.me)], self.m[k], self.v[k])
            for i, (source, target) in enumerate(zip(sources, (self.own, self.m_in, self.v_in), strict=True)):
                pltpu.make_async_copy(source, target.at[mine], self.state_sem.at[i]).start()

    def states_loaded(self):
        for i, whole in enumerate((self.own, self.m_in, self.v_in)):
            pltpu.make_async_copy(whole, whole, self.state_sem.at[i]).wait()

    def remote(self, side, source, target, recv_sem):
        return pltpu.make_async_remote_copy(
            src_ref=source,
            dst_ref=target,
            send_sem=self.send_sem.at[side],
            recv_sem=self.recv_sem.at[recv_sem],
            device_id={"dp": self.to[side]},
            device_id_type=MESH,
        )

    def sum_copy(self, p, side, left):
        away = left if side == 0 else -left
        if self.hops[p][side] == left:
            k, layer, *_ = self.parts[p]
            source = self.g[k].at[0, layer, self.rows(p, self.at(away))]
        else:
            source = self.term(p, away)
        return self.remote(side, source, self.came(p, side, left), self.message[p, side, left])

    def gather_copy(self, p, side, hop, back, done=None):
        away = hop - back
        k, layer, *_ = self.parts[p]
        block = (layer, self.rows(p, self.at(-away if side == 0 else away)))
        return self.remote(side, (done or self.w_out)[k].at[block], self.w_out[k].at[block], self.message[p, side, self.hops[p][side] + 1 - hop])

    def live(self, side, hops):
        return [p for p in range(self.pieces) if self.hops[p][side] >= hops]

    def first_terms(self):
        for left in range(self.far, 0, -1):
            for order in zip(*([p for p in range(self.pieces) if self.hops[p][s] == left] for s in (0, 1)), strict=True):
                for s, p in enumerate(order):
                    self.sum_copy(p, s, left).start()

    def pass_on(self):
        for left in range(self.far - 1, 0, -1):
            for order in zip(*(self.live(s, left + 1) for s in (0, 1)), strict=True):
                for s, p in enumerate(order):
                    away = left if s == 0 else -left
                    self.loaded(away)
                    self.sum_copy(p, s, left + 1).wait_recv()
                    here, came = self.term(p, away), self.came(p, s, left + 1)

                    def add(r, here=here, came=came):
                        r = pl.ds(r, ROWS)
                        here[r, :] = (here[r, :].astype(jnp.float32) + came[r, :].astype(jnp.float32)).astype(jnp.bfloat16)

                    by_rows(self.parts[p][3], add)
                    self.sum_copy(p, s, left).start()

    def finish_sum(self, p):
        for s in (0, 1):
            self.sum_copy(p, s, 1).wait_recv()
        _, _, first, count = self.parts[p]

        def add(r):
            here = pl.ds(r, ROWS)
            parts = [ref[here, :].astype(jnp.float32) for ref in (self.term(p, 0), self.came(p, 0, 1), self.came(p, 1, 1))]
            self.total.at[self.matrix(p)][pl.ds(first + r, ROWS), :] = (parts[0] + parts[1] + parts[2]).astype(jnp.bfloat16)

        by_rows(count, add)

    def step(self, p):
        k, layer, first, count = self.parts[p]

        def take(r):
            rows = pl.ds(first + r, ROWS)
            w, m, v, g = (ref.at[self.matrix(p)][rows, :] for ref in (self.own, self.m_in, self.v_in, self.total))
            new = adamw(w.astype(jnp.float32), m, v, g.astype(jnp.float32))
            self.w_out[k].at[layer][pl.ds(pl.multiple_of(self.me * self.block_rows + (first + r), ROWS), ROWS), :] = new[0]
            self.m_out[k].at[layer][rows, :] = new[1]
            self.v_out[k].at[layer][rows, :] = new[2]

        by_rows(count, take)
        for s in (0, 1):
            self.gather_copy(p, s, 1, 1).start()

    def take_steps(self):
        self.loaded(0)
        self.states_loaded()
        for p in range(self.pieces):
            self.finish_sum(p)
            self.step(p)

    def spread(self, hop, done=None):
        order = [self.live(s, hop) for s in (0, 1)]
        for s in (0, 1):
            if hop == self.far - 1:
                order[s].sort(key=lambda p, s=s: -self.hops[p][s])
        for pair in zip(*order, strict=True):
            for s, p in enumerate(pair):
                if done is None:
                    self.gather_copy(p, s, hop - 1, 0).wait_recv()
                self.gather_copy(p, s, hop, 1, done).start()

    def gathered(self, hops):
        for hop in range(1, hops + 1):
            for p in range(self.pieces):
                for s in (0, 1):
                    if min(self.hops[p][s], hops) == hop:
                        self.gather_copy(p, s, hop, 0).wait_recv()

    def all_sent(self, hops, sums):
        for s in (0, 1):
            rows = sum(self.parts[p][3] for hop in hops for p in self.live(s, hop)) + sums * self.inbox_rows
            whole = self.inbox.at[pl.ds(0, rows)]
            pltpu.make_async_copy(whole, whole, self.send_sem.at[s]).wait()

    def greet(self):
        barrier = pltpu.get_barrier_semaphore()
        for neighbour in self.to:
            pl.semaphore_signal(barrier, inc=1, device_id={"dp": neighbour}, device_id_type=MESH)
        pl.semaphore_wait(barrier, 2)


def ahead():
    return lax.rem(lax.axis_index("rep"), 2) == 0


def behind():
    return lax.rem(lax.axis_index("rep"), 2) == 1


def early_hops(n):
    return n // 2 - 2


def early_kernel(n, shape, late_shape, *refs):
    refs = list(refs)
    take = lambda c: [refs.pop(0) for _ in range(c)]
    e, l = shape[0], late_shape[0]
    data, late_data = [take(e) for _ in range(4)], [take(l) for _ in range(4)]
    results, late_results = [take(e) for _ in range(3)], [take(l) for _ in range(3)]
    me = lax.axis_index("dp")
    ring = Ring(n, me, shape, EARLY_PIECES, *data, results, take(6), take(4))
    late = Ring(n, me, late_shape, LATE_PIECES, *late_data, late_results, take(6), take(4))

    ring.greet()
    pl.when(ahead())(late.first_terms)
    ring.first_terms()

    @pl.when(ahead())
    def _():
        late.load_terms()
        late.load_states()

    ring.load_terms()
    ring.load_states()

    @pl.when(ahead())
    def _():
        late.pass_on()
        late.take_steps()

    ring.pass_on()
    ring.take_steps()
    for hop in range(2, ring.far + 1):
        if hop <= early_hops(n):
            pl.when(ahead())(functools.partial(late.spread, hop))
        ring.spread(hop)
    ring.gathered(ring.far)
    ring.all_sent(range(1, ring.far + 1), True)

    @pl.when(ahead())
    def _():
        late.gathered(early_hops(n))
        late.all_sent(range(1, early_hops(n) + 1), True)


def late_kernel(n, shape, *refs):
    refs = list(refs)
    take = lambda c: [refs.pop(0) for _ in range(c)]
    count = shape[0]
    data, done = [take(count) for _ in range(4)], take(count)
    results = [take(count) for _ in range(3)]
    ring = Ring(n, lax.axis_index("dp"), shape, LATE_PIECES, *data, results, take(6), take(4))
    last = range(early_hops(n) + 1, ring.far + 1)
    ring.greet()

    @pl.when(ahead())
    def _():
        pl.delay(HOLD)
        ring.spread(last[0], done)

    @pl.when(behind())
    def _():
        ring.first_terms()
        ring.load_terms()
        ring.load_states()
        ring.pass_on()
        ring.take_steps()
        for hop in range(2, last[0] + 1):
            ring.spread(hop)

    for hop in last[1:]:
        ring.spread(hop)
    ring.gathered(ring.far)
    pl.when(ahead())(functools.partial(ring.all_sent, last, False))
    pl.when(behind())(functools.partial(ring.all_sent, range(1, ring.far + 1), True))


def put_early_kernel(n, e, l, *refs):
    refs, sem = list(refs[:-1]), refs[-1]
    count = 3 * (e + l)
    sources, results = refs[:count], refs[count:]
    early = [pltpu.make_async_copy(sources[i], results[i], sem.at[i]) for i in range(3 * e)]
    for copy in early:
        copy.start()

    @pl.when(ahead())
    def _():
        reach = early_hops(n)
        late = [pltpu.make_async_copy(sources[i], results[i], sem.at[i]) for i in range(3 * e + l, count)]
        late += block_copies(n, sources[3 * e : 3 * e + l], results[3 * e : 3 * e + l], range(-reach, reach + 1), sem, count)
        for copy in late:
            copy.start()
        for copy in late:
            copy.wait()

    for copy in early:
        copy.wait()


def block_copies(n, sources, results, aways, sem, first):
    me = lax.axis_index("dp")
    copies = []
    for source, result in zip(sources, results, strict=True):
        rows = source.shape[1] // n
        for away in aways:
            block = pl.ds(pl.multiple_of(lax.rem(me + (away + n), n) * rows, rows), rows)
            copies.append(pltpu.make_async_copy(source.at[:, block], result.at[:, block], sem.at[first + len(copies)]))
    return copies


def put_late_kernel(n, l, *refs):
    sources, results, sem = refs[: 3 * l], refs[6 * l : 9 * l], refs[-1]

    @pl.when(ahead())
    def _():
        reach = early_hops(n)
        copies = block_copies(n, sources[:l], results[:l], range(reach + 1, n - reach), sem, 3 * l)
        for copy in copies:
            copy.start()
        for copy in copies:
            copy.wait()

    @pl.when(behind())
    def _():
        copies = [pltpu.make_async_copy(sources[i], results[i], sem.at[i]) for i in range(3 * l)]
        for copy in copies:
            copy.start()
        for copy in copies:
            copy.wait()


def solution(mesh):
    n = mesh.shape["dp"]

    def step(*arrays):
        g, w, m, v = (arrays[i : i + 3] for i in (0, 3, 6, 9))
        early, late = slice(0, 2), slice(2, 3)
        e, l = len(g[early]), len(g[late])
        vmem = lambda several: [pltpu.VMEM(one.shape, one.dtype) for one in several]
        hbm = lambda several: [pltpu.HBM(one.shape, one.dtype) for one in several]
        early_shape, late_shape = (e, *m[early][0].shape), (l, *m[late][0].shape)
        early_results, late_results = (*w[early], *m[early], *v[early]), (*w[late], *m[late], *v[late])

        first = pl.pallas_call(
            functools.partial(early_kernel, n, early_shape, late_shape),
            out_shape=vmem((*early_results, *late_results)),
            in_specs=[HBM] * (4 * (e + l)),
            out_specs=[VMEM] * (3 * (e + l)),
            scratch_shapes=[*Ring.scratch(n, EARLY_PIECES, early_shape), *Ring.scratch(n, LATE_PIECES, late_shape)],
            compiler_params=pltpu.CompilerParams(collective_id=0, has_side_effects=True, vmem_limit_bytes=GRANT_EARLY),
        )(*g[early], *w[early], *m[early], *v[early], *g[late], *w[late], *m[late], *v[late])
        first = pl.pallas_call(
            functools.partial(put_early_kernel, n, e, l),
            out_shape=hbm((*early_results, *late_results)),
            in_specs=[VMEM] * (3 * (e + l)),
            out_specs=[HBM] * (3 * (e + l)),
            scratch_shapes=[DMA((3 * (e + l) + l * (2 * early_hops(n) + 1),))],
            compiler_params=pltpu.CompilerParams(vmem_limit_bytes=1 << 20),
        )(*first)
        first, half = first[: 3 * e], first[3 * e :]
        second = pl.pallas_call(
            functools.partial(late_kernel, n, late_shape),
            out_shape=vmem(late_results),
            in_specs=[HBM] * (5 * l),
            out_specs=[VMEM] * (3 * l),
            scratch_shapes=Ring.scratch(n, LATE_PIECES, late_shape),
            compiler_params=pltpu.CompilerParams(collective_id=1, has_side_effects=True, vmem_limit_bytes=GRANT_LATE),
        )(*g[late], *w[late], *m[late], *v[late], *half[:l])
        second = pl.pallas_call(
            functools.partial(put_late_kernel, n, l),
            out_shape=hbm(late_results),
            in_specs=[VMEM] * (3 * l) + [HBM] * (3 * l),
            out_specs=[HBM] * (3 * l),
            scratch_shapes=[DMA((3 * l + l * (n - 1 - 2 * early_hops(n)),))],
            input_output_aliases={3 * l + i: i for i in range(3 * l)},
            compiler_params=pltpu.CompilerParams(vmem_limit_bytes=1 << 20),
        )(*second, *half)
        return tuple(one for i in range(3) for one in (*first[i * e : (i + 1) * e], *second[i * l : (i + 1) * l]))

    all_of, cut = P(None, None, None), P(None, "dp", None)
    return jax.shard_map(
        step,
        mesh=mesh,
        in_specs=(P(("rep", "dp"), None, None, None),) * 3 + (all_of,) * 3 + (cut,) * 6,
        out_specs=(P("rep", None, None),) * 3 + (P("rep", "dp", None),) * 6,
        check_vma=False,
    )
```

```python
import functools

import jax
import jax.numpy as jnp
from jax import lax
from jax.experimental import pallas as pl
from jax.experimental.pallas import tpu as pltpu
from jax.sharding import PartitionSpec as P

MESH = pl.DeviceIdType.MESH
DMA = pltpu.SemaphoreType.DMA
HBM, VMEM = pl.BlockSpec(memory_space=pltpu.HBM), pl.BlockSpec(memory_space=pltpu.VMEM)
ROWS = 16
EARLY_PIECES, LATE_PIECES = 1, 2
HOLD = 3200
GRANT_EARLY, GRANT_LATE = 54_000_000, 61_500_000


def adamw(w, m, v, g):
    m = 0.9 * m + 0.1 * g
    v = 0.95 * v + 0.05 * g * g
    step = m * lax.rsqrt(v + 1e-8) + 0.1 * w
    return (w - 0.02 * step).astype(jnp.bfloat16), m, v


def by_rows(count, body):
    lax.fori_loop(0, count // ROWS, lambda i, _: body(pl.multiple_of(i * ROWS, ROWS)), None)


class Ring:
    def __init__(self, n, me, shape, pieces, g, w, m, v, results, buffers, sems):
        self.n, self.me, self.g, self.w, self.m, self.v = n, me, g, w, m, v
        self.w_out, self.m_out, self.v_out = results
        self.terms, self.inbox, self.total, self.own, self.m_in, self.v_in = buffers
        self.load_sem, self.state_sem, self.send_sem, self.recv_sem = sems
        self.to = [lax.rem(me + 1, n), lax.rem(me + n - 1, n)]
        weights, self.layers, self.block_rows, _ = shape
        self.parts, self.hops, self.place, self.inbox_rows, self.message, _ = self.cut(n, pieces, shape)
        self.pieces = len(self.parts)
        self.far = n // 2
        self.loads_over = set()

    @staticmethod
    def cut(n, pieces, shape):
        weights, layers, rows, _ = shape
        size = -(-rows // (pieces * ROWS)) * ROWS
        parts, hops, place, message = [], [], {}, {}
        end = [0, 0]
        for k in range(weights):
            for layer in range(layers):
                for i, r in enumerate(range(0, rows, size)):
                    p, count = len(parts), min(size, rows - r)
                    parts.append((k, layer, r, count))
                    ways = (n // 2, (n - 1) // 2)
                    hops.append(ways if (i + layer) % 2 == 0 else ways[::-1])
                    for s in (0, 1):
                        for left in range(1, hops[p][s] + 1):
                            place[p, s, left] = end[s]
                            end[s] += count
                            message[p, s, left] = len(message)
        assert end[0] == end[1]
        return parts, hops, place, end[0], message, len(message)

    @classmethod
    def scratch(cls, n, pieces, shape):
        weights, layers, rows, columns = shape
        _, _, _, inbox_rows, _, messages = cls.cut(n, pieces, shape)
        whole = (weights * layers, rows, columns)
        data = [pltpu.VMEM((n, *whole), jnp.bfloat16), pltpu.VMEM((2 * inbox_rows, columns), jnp.bfloat16)]
        data += [pltpu.VMEM(whole, t) for t in (jnp.bfloat16, jnp.bfloat16, jnp.float32, jnp.float32)]
        return [*data, DMA((n,)), DMA((3,)), DMA((2,)), DMA((messages,))]

    def at(self, away):
        return lax.rem(self.me + (away + self.n), self.n)

    def block(self, owner):
        return pl.ds(pl.multiple_of(owner * self.block_rows, self.block_rows), self.block_rows)

    def rows(self, p, owner):
        _, _, first, count = self.parts[p]
        return pl.ds(pl.multiple_of(owner * self.block_rows + first, ROWS), count)

    def matrix(self, p):
        k, layer, *_ = self.parts[p]
        return k * self.layers + layer

    def term(self, p, away):
        _, _, first, count = self.parts[p]
        return self.terms.at[away % self.n, self.matrix(p), pl.ds(first, count)]

    def came(self, p, side, left):
        return self.inbox.at[pl.ds(side * self.inbox_rows + self.place[p, side, left], self.parts[p][3])]

    def load_terms(self):
        for left in range(self.far - 1, -1, -1):
            for away in sorted({left, -left}):
                for k, g in enumerate(self.g):
                    target = self.terms.at[away % self.n, pl.ds(k * self.layers, self.layers)]
                    pltpu.make_async_copy(g.at[0, :, self.block(self.at(away))], target, self.load_sem.at[away % self.n]).start()

    def loaded(self, away):
        if away not in self.loads_over:
            self.loads_over.add(away)
            whole = self.terms.at[away % self.n]
            pltpu.make_async_copy(whole, whole, self.load_sem.at[away % self.n]).wait()

    def load_states(self):
        for k in range(len(self.g)):
            mine = pl.ds(k * self.layers, self.layers)
            sources = (self.w[k].at[:, self.block(self.me)], self.m[k], self.v[k])
            for i, (source, target) in enumerate(zip(sources, (self.own, self.m_in, self.v_in), strict=True)):
                pltpu.make_async_copy(source, target.at[mine], self.state_sem.at[i]).start()

    def states_loaded(self):
        for i, whole in enumerate((self.own, self.m_in, self.v_in)):
            pltpu.make_async_copy(whole, whole, self.state_sem.at[i]).wait()

    def remote(self, side, source, target, recv_sem):
        return pltpu.make_async_remote_copy(
            src_ref=source,
            dst_ref=target,
            send_sem=self.send_sem.at[side],
            recv_sem=self.recv_sem.at[recv_sem],
            device_id={"dp": self.to[side]},
            device_id_type=MESH,
        )

    def sum_copy(self, p, side, left):
        away = left if side == 0 else -left
        if self.hops[p][side] == left:
            k, layer, *_ = self.parts[p]
            source = self.g[k].at[0, layer, self.rows(p, self.at(away))]
        else:
            source = self.term(p, away)
        return self.remote(side, source, self.came(p, side, left), self.message[p, side, left])

    def gather_copy(self, p, side, hop, back, done=None):
        away = hop - back
        k, layer, *_ = self.parts[p]
        block = (layer, self.rows(p, self.at(-away if side == 0 else away)))
        return self.remote(side, (done or self.w_out)[k].at[block], self.w_out[k].at[block], self.message[p, side, self.hops[p][side] + 1 - hop])

    def live(self, side, hops):
        return [p for p in range(self.pieces) if self.hops[p][side] >= hops]

    def first_terms(self):
        for left in range(self.far, 0, -1):
            for order in zip(*([p for p in range(self.pieces) if self.hops[p][s] == left] for s in (0, 1)), strict=True):
                for s, p in enumerate(order):
                    self.sum_copy(p, s, left).start()

    def pass_on(self):
        for left in range(self.far - 1, 0, -1):
            for order in zip(*(self.live(s, left + 1) for s in (0, 1)), strict=True):
                for s, p in enumerate(order):
                    away = left if s == 0 else -left
                    self.loaded(away)
                    self.sum_copy(p, s, left + 1).wait_recv()
                    here, came = self.term(p, away), self.came(p, s, left + 1)

                    def add(r, here=here, came=came):
                        r = pl.ds(r, ROWS)
                        here[r, :] = (here[r, :].astype(jnp.float32) + came[r, :].astype(jnp.float32)).astype(jnp.bfloat16)

                    by_rows(self.parts[p][3], add)
                    self.sum_copy(p, s, left).start()

    def finish_sum(self, p):
        for s in (0, 1):
            self.sum_copy(p, s, 1).wait_recv()
        _, _, first, count = self.parts[p]

        def add(r):
            here = pl.ds(r, ROWS)
            parts = [ref[here, :].astype(jnp.float32) for ref in (self.term(p, 0), self.came(p, 0, 1), self.came(p, 1, 1))]
            self.total.at[self.matrix(p)][pl.ds(first + r, ROWS), :] = (parts[0] + parts[1] + parts[2]).astype(jnp.bfloat16)

        by_rows(count, add)

    def step(self, p):
        k, layer, first, count = self.parts[p]

        def take(r):
            rows = pl.ds(first + r, ROWS)
            w, m, v, g = (ref.at[self.matrix(p)][rows, :] for ref in (self.own, self.m_in, self.v_in, self.total))
            new = adamw(w.astype(jnp.float32), m, v, g.astype(jnp.float32))
            self.w_out[k].at[layer][pl.ds(pl.multiple_of(self.me * self.block_rows + (first + r), ROWS), ROWS), :] = new[0]
            self.m_out[k].at[layer][rows, :] = new[1]
            self.v_out[k].at[layer][rows, :] = new[2]

        by_rows(count, take)
        for s in (0, 1):
            self.gather_copy(p, s, 1, 1).start()

    def take_steps(self):
        self.loaded(0)
        self.states_loaded()
        for p in range(self.pieces):
            self.finish_sum(p)
            self.step(p)

    def spread(self, hop, spare=0):
        order = [self.live(s, hop + spare) for s in (0, 1)]
        for s in (0, 1):
            if hop == self.far - 1:
                order[s].sort(key=lambda p, s=s: -self.hops[p][s])
        for pair in zip(*order, strict=True):
            for s, p in enumerate(pair):
                self.gather_copy(p, s, hop - 1, 0).wait_recv()
                self.gather_copy(p, s, hop, 1).start()

    def last_hops(self, done):
        for p in range(self.pieces):
            for s in (0, 1):
                self.gather_copy(p, s, self.hops[p][s], 1, done).start()

    def gathered(self, spare):
        for hop in (self.far - 1, self.far):
            for p in range(self.pieces):
                for s in (0, 1):
                    if self.hops[p][s] == hop:
                        self.gather_copy(p, s, hop - spare, 0).wait_recv()

    def way_rows(self, spare):
        return sum((hops[0] - spare) * part[3] for hops, part in zip(self.hops, self.parts, strict=True))

    def all_sent(self, rows):
        for s in (0, 1):
            whole = self.inbox.at[pl.ds(0, rows)]
            pltpu.make_async_copy(whole, whole, self.send_sem.at[s]).wait()

    def greet(self):
        barrier = pltpu.get_barrier_semaphore()
        for neighbour in self.to:
            pl.semaphore_signal(barrier, inc=1, device_id={"dp": neighbour}, device_id_type=MESH)
        pl.semaphore_wait(barrier, 2)


def ahead():
    return lax.rem(lax.axis_index("rep"), 2) == 0


def behind():
    return lax.rem(lax.axis_index("rep"), 2) == 1


def early_kernel(n, shape, late_shape, *refs):
    refs = list(refs)
    take = lambda c: [refs.pop(0) for _ in range(c)]
    e, l = shape[0], late_shape[0]
    data, late_data = [take(e) for _ in range(4)], [take(l) for _ in range(4)]
    results, late_results = [take(e) for _ in range(3)], [take(l) for _ in range(3)]
    me = lax.axis_index("dp")
    ring = Ring(n, me, shape, EARLY_PIECES, *data, results, take(6), take(4))
    late = Ring(n, me, late_shape, LATE_PIECES, *late_data, late_results, take(6), take(4))

    ring.greet()
    pl.when(ahead())(late.first_terms)
    ring.first_terms()

    @pl.when(ahead())
    def _():
        late.load_terms()
        late.load_states()

    ring.load_terms()
    ring.load_states()

    @pl.when(ahead())
    def _():
        late.pass_on()
        late.take_steps()

    ring.pass_on()
    ring.take_steps()
    for hop in range(2, ring.far + 1):
        if hop < ring.far:
            pl.when(ahead())(functools.partial(late.spread, hop, 1))
        ring.spread(hop)
    ring.gathered(0)
    ring.all_sent(ring.way_rows(0) + ring.inbox_rows)

    @pl.when(ahead())
    def _():
        late.gathered(1)
        late.all_sent(late.way_rows(1) + late.inbox_rows)


def late_kernel(n, shape, *refs):
    refs = list(refs)
    take = lambda c: [refs.pop(0) for _ in range(c)]
    count = shape[0]
    data, done = [take(count) for _ in range(4)], take(count)
    results = [take(count) for _ in range(3)]
    ring = Ring(n, lax.axis_index("dp"), shape, LATE_PIECES, *data, results, take(6), take(4))
    ring.greet()

    @pl.when(ahead())
    def _():
        pl.delay(HOLD)
        ring.last_hops(done)

    @pl.when(behind())
    def _():
        ring.first_terms()
        ring.load_terms()
        ring.load_states()
        ring.pass_on()
        ring.take_steps()
        for hop in range(2, ring.far + 1):
            ring.spread(hop)

    ring.gathered(0)
    pl.when(ahead())(functools.partial(ring.all_sent, ring.way_rows(0) - ring.way_rows(1)))
    pl.when(behind())(functools.partial(ring.all_sent, ring.way_rows(0) + ring.inbox_rows))


def parted(n, shape, last):
    weights, _, rows, _ = shape
    parts, hops, *_ = Ring.cut(n, LATE_PIECES, shape)
    far, near = n // 2, (n - 1) // 2
    whole = [far] if last else range(1 - near, near)
    wanted = [(k, None, 0, rows, away) for k in range(weights) for away in whole]
    for p, (k, layer, first, count) in enumerate(parts):
        from_before = (hops[p][0] == far) != last
        wanted.append((k, layer, first, count, -near if from_before else near))
    return wanted


def put_early_kernel(n, e, shape, *refs):
    refs, sem = list(refs[:-1]), refs[-1]
    l = shape[0]
    count = 3 * (e + l)
    sources, results = refs[:count], refs[count:]
    early = [pltpu.make_async_copy(sources[i], results[i], sem.at[i]) for i in range(3 * e)]
    for copy in early:
        copy.start()

    @pl.when(ahead())
    def _():
        late = [pltpu.make_async_copy(sources[i], results[i], sem.at[i]) for i in range(3 * e + l, count)]
        late += block_copies(n, sources[3 * e : 3 * e + l], results[3 * e : 3 * e + l], parted(n, shape, False), sem, count)
        for copy in late:
            copy.start()
        for copy in late:
            copy.wait()

    for copy in early:
        copy.wait()


def block_copies(n, sources, results, wanted, sem, first_sem):
    me = lax.axis_index("dp")
    copies = []
    for k, layer, first, count, away in wanted:
        block_rows = sources[k].shape[1] // n
        rows = pl.ds(pl.multiple_of(lax.rem(me + (away + n), n) * block_rows + first, ROWS), count)
        at = (slice(None) if layer is None else layer, rows)
        copies.append(pltpu.make_async_copy(sources[k].at[at], results[k].at[at], sem.at[first_sem + len(copies)]))
    return copies


def put_late_kernel(n, shape, *refs):
    l = shape[0]
    sources, results, sem = refs[: 3 * l], refs[6 * l : 9 * l], refs[-1]

    @pl.when(ahead())
    def _():
        copies = block_copies(n, sources[:l], results[:l], parted(n, shape, True), sem, 3 * l)
        for copy in copies:
            copy.start()
        for copy in copies:
            copy.wait()

    @pl.when(behind())
    def _():
        copies = [pltpu.make_async_copy(sources[i], results[i], sem.at[i]) for i in range(3 * l)]
        for copy in copies:
            copy.start()
        for copy in copies:
            copy.wait()


def solution(mesh):
    n = mesh.shape["dp"]

    def step(*arrays):
        g, w, m, v = (arrays[i : i + 3] for i in (0, 3, 6, 9))
        early, late = slice(0, 2), slice(2, 3)
        e, l = len(g[early]), len(g[late])
        vmem = lambda several: [pltpu.VMEM(one.shape, one.dtype) for one in several]
        hbm = lambda several: [pltpu.HBM(one.shape, one.dtype) for one in several]
        early_shape, late_shape = (e, *m[early][0].shape), (l, *m[late][0].shape)
        early_results, late_results = (*w[early], *m[early], *v[early]), (*w[late], *m[late], *v[late])

        first = pl.pallas_call(
            functools.partial(early_kernel, n, early_shape, late_shape),
            out_shape=vmem((*early_results, *late_results)),
            in_specs=[HBM] * (4 * (e + l)),
            out_specs=[VMEM] * (3 * (e + l)),
            scratch_shapes=[*Ring.scratch(n, EARLY_PIECES, early_shape), *Ring.scratch(n, LATE_PIECES, late_shape)],
            compiler_params=pltpu.CompilerParams(collective_id=0, has_side_effects=True, vmem_limit_bytes=GRANT_EARLY),
        )(*g[early], *w[early], *m[early], *v[early], *g[late], *w[late], *m[late], *v[late])
        first = pl.pallas_call(
            functools.partial(put_early_kernel, n, e, late_shape),
            out_shape=hbm((*early_results, *late_results)),
            in_specs=[VMEM] * (3 * (e + l)),
            out_specs=[HBM] * (3 * (e + l)),
            scratch_shapes=[DMA((3 * (e + l) + len(parted(n, late_shape, False)),))],
            compiler_params=pltpu.CompilerParams(vmem_limit_bytes=1 << 20),
        )(*first)
        first, half = first[: 3 * e], first[3 * e :]
        second = pl.pallas_call(
            functools.partial(late_kernel, n, late_shape),
            out_shape=vmem(late_results),
            in_specs=[HBM] * (5 * l),
            out_specs=[VMEM] * (3 * l),
            scratch_shapes=Ring.scratch(n, LATE_PIECES, late_shape),
            compiler_params=pltpu.CompilerParams(collective_id=1, has_side_effects=True, vmem_limit_bytes=GRANT_LATE),
        )(*g[late], *w[late], *m[late], *v[late], *half[:l])
        second = pl.pallas_call(
            functools.partial(put_late_kernel, n, late_shape),
            out_shape=hbm(late_results),
            in_specs=[VMEM] * (3 * l) + [HBM] * (3 * l),
            out_specs=[HBM] * (3 * l),
            scratch_shapes=[DMA((3 * l + len(parted(n, late_shape, True)),))],
            input_output_aliases={3 * l + i: i for i in range(3 * l)},
            compiler_params=pltpu.CompilerParams(vmem_limit_bytes=1 << 20),
        )(*second, *half)
        return tuple(one for i in range(3) for one in (*first[i * e : (i + 1) * e], *second[i * l : (i + 1) * l]))

    all_of, cut = P(None, None, None), P(None, "dp", None)
    return jax.shard_map(
        step,
        mesh=mesh,
        in_specs=(P(("rep", "dp"), None, None, None),) * 3 + (all_of,) * 3 + (cut,) * 6,
        out_specs=(P("rep", None, None),) * 3 + (P("rep", "dp", None),) * 6,
        check_vma=False,
    )
```

```python
import functools

import jax
import jax.numpy as jnp
from jax import lax
from jax.experimental import pallas as pl
from jax.experimental.pallas import tpu as pltpu
from jax.sharding import PartitionSpec as P

MESH = pl.DeviceIdType.MESH
DMA = pltpu.SemaphoreType.DMA
HBM, VMEM = pl.BlockSpec(memory_space=pltpu.HBM), pl.BlockSpec(memory_space=pltpu.VMEM)
ROWS = 16
EARLY_PIECES, LATE_PIECES = 1, 4
HOLD = 900
GRANT_EARLY, GRANT_LATE = 54_000_000, 61_500_000


def adamw(w, m, v, g):
    m = 0.9 * m + 0.1 * g
    v = 0.95 * v + 0.05 * g * g
    step = m * lax.rsqrt(v + 1e-8) + 0.1 * w
    return (w - 0.02 * step).astype(jnp.bfloat16), m, v


def by_rows(count, body):
    lax.fori_loop(0, count // ROWS, lambda i, _: body(pl.multiple_of(i * ROWS, ROWS)), None)


class Ring:
    def __init__(self, n, me, shape, pieces, g, w, m, v, results, buffers, sems):
        self.n, self.me, self.g, self.w, self.m, self.v = n, me, g, w, m, v
        self.w_out, self.m_out, self.v_out = results
        self.terms, self.inbox, self.total, self.own, self.m_in, self.v_in = buffers
        self.load_sem, self.state_sem, self.send_sem, self.recv_sem = sems
        self.to = [lax.rem(me + 1, n), lax.rem(me + n - 1, n)]
        weights, self.layers, self.block_rows, _ = shape
        self.parts, self.hops, self.place, self.inbox_rows, self.message, _ = self.cut(n, pieces, shape)
        self.pieces = len(self.parts)
        self.far = n // 2
        self.loads_over = set()

    @staticmethod
    def cut(n, pieces, shape):
        weights, layers, rows, _ = shape
        size = -(-rows // (pieces * ROWS)) * ROWS
        parts, hops, place, message = [], [], {}, {}
        end = [0, 0]
        for k in range(weights):
            for layer in range(layers):
                for i, r in enumerate(range(0, rows, size)):
                    p, count = len(parts), min(size, rows - r)
                    parts.append((k, layer, r, count))
                    ways = (n // 2, (n - 1) // 2)
                    hops.append(ways if (i + layer) % 2 == 0 else ways[::-1])
                    for s in (0, 1):
                        for left in range(1, hops[p][s] + 1):
                            place[p, s, left] = end[s]
                            end[s] += count
                            message[p, s, left] = len(message)
        assert end[0] == end[1]
        return parts, hops, place, end[0], message, len(message)

    @classmethod
    def scratch(cls, n, pieces, shape):
        weights, layers, rows, columns = shape
        _, _, _, inbox_rows, _, messages = cls.cut(n, pieces, shape)
        whole = (weights * layers, rows, columns)
        data = [pltpu.VMEM((n, *whole), jnp.bfloat16), pltpu.VMEM((2 * inbox_rows, columns), jnp.bfloat16)]
        data += [pltpu.VMEM(whole, t) for t in (jnp.bfloat16, jnp.bfloat16, jnp.float32, jnp.float32)]
        return [*data, DMA((n,)), DMA((3,)), DMA((2,)), DMA((messages,))]

    def at(self, away):
        return lax.rem(self.me + (away + self.n), self.n)

    def block(self, owner):
        return pl.ds(pl.multiple_of(owner * self.block_rows, self.block_rows), self.block_rows)

    def rows(self, p, owner):
        _, _, first, count = self.parts[p]
        return pl.ds(pl.multiple_of(owner * self.block_rows + first, ROWS), count)

    def matrix(self, p):
        k, layer, *_ = self.parts[p]
        return k * self.layers + layer

    def term(self, p, away):
        _, _, first, count = self.parts[p]
        return self.terms.at[away % self.n, self.matrix(p), pl.ds(first, count)]

    def came(self, p, side, left):
        return self.inbox.at[pl.ds(side * self.inbox_rows + self.place[p, side, left], self.parts[p][3])]

    def load_terms(self):
        for left in range(self.far - 1, -1, -1):
            for away in sorted({left, -left}):
                for k, g in enumerate(self.g):
                    target = self.terms.at[away % self.n, pl.ds(k * self.layers, self.layers)]
                    pltpu.make_async_copy(g.at[0, :, self.block(self.at(away))], target, self.load_sem.at[away % self.n]).start()

    def loaded(self, away):
        if away not in self.loads_over:
            self.loads_over.add(away)
            whole = self.terms.at[away % self.n]
            pltpu.make_async_copy(whole, whole, self.load_sem.at[away % self.n]).wait()

    def load_states(self):
        for k in range(len(self.g)):
            mine = pl.ds(k * self.layers, self.layers)
            sources = (self.w[k].at[:, self.block(self.me)], self.m[k], self.v[k])
            for i, (source, target) in enumerate(zip(sources, (self.own, self.m_in, self.v_in), strict=True)):
                pltpu.make_async_copy(source, target.at[mine], self.state_sem.at[i]).start()

    def states_loaded(self):
        for i, whole in enumerate((self.own, self.m_in, self.v_in)):
            pltpu.make_async_copy(whole, whole, self.state_sem.at[i]).wait()

    def remote(self, side, source, target, recv_sem):
        return pltpu.make_async_remote_copy(
            src_ref=source,
            dst_ref=target,
            send_sem=self.send_sem.at[side],
            recv_sem=self.recv_sem.at[recv_sem],
            device_id={"dp": self.to[side]},
            device_id_type=MESH,
        )

    def sum_copy(self, p, side, left):
        away = left if side == 0 else -left
        if self.hops[p][side] == left:
            k, layer, *_ = self.parts[p]
            source = self.g[k].at[0, layer, self.rows(p, self.at(away))]
        else:
            source = self.term(p, away)
        return self.remote(side, source, self.came(p, side, left), self.message[p, side, left])

    def gather_copy(self, p, side, hop, back, done=None):
        away = hop - back
        k, layer, *_ = self.parts[p]
        block = (layer, self.rows(p, self.at(-away if side == 0 else away)))
        return self.remote(side, (done or self.w_out)[k].at[block], self.w_out[k].at[block], self.message[p, side, self.hops[p][side] + 1 - hop])

    def live(self, side, hops):
        return [p for p in range(self.pieces) if self.hops[p][side] >= hops]

    def first_terms(self):
        for left in range(self.far, 0, -1):
            for order in zip(*([p for p in range(self.pieces) if self.hops[p][s] == left] for s in (0, 1)), strict=True):
                for s, p in enumerate(order):
                    self.sum_copy(p, s, left).start()

    def pass_on(self):
        for left in range(self.far - 1, 0, -1):
            for order in zip(*(self.live(s, left + 1) for s in (0, 1)), strict=True):
                for s, p in enumerate(order):
                    away = left if s == 0 else -left
                    self.loaded(away)
                    self.sum_copy(p, s, left + 1).wait_recv()
                    here, came = self.term(p, away), self.came(p, s, left + 1)

                    def add(r, here=here, came=came):
                        r = pl.ds(r, ROWS)
                        here[r, :] = (here[r, :].astype(jnp.float32) + came[r, :].astype(jnp.float32)).astype(jnp.bfloat16)

                    by_rows(self.parts[p][3], add)
                    self.sum_copy(p, s, left).start()

    def finish_sum(self, p):
        for s in (0, 1):
            self.sum_copy(p, s, 1).wait_recv()
        _, _, first, count = self.parts[p]

        def add(r):
            here = pl.ds(r, ROWS)
            parts = [ref[here, :].astype(jnp.float32) for ref in (self.term(p, 0), self.came(p, 0, 1), self.came(p, 1, 1))]
            self.total.at[self.matrix(p)][pl.ds(first + r, ROWS), :] = (parts[0] + parts[1] + parts[2]).astype(jnp.bfloat16)

        by_rows(count, add)

    def step(self, p):
        k, layer, first, count = self.parts[p]

        def take(r):
            rows = pl.ds(first + r, ROWS)
            w, m, v, g = (ref.at[self.matrix(p)][rows, :] for ref in (self.own, self.m_in, self.v_in, self.total))
            new = adamw(w.astype(jnp.float32), m, v, g.astype(jnp.float32))
            self.w_out[k].at[layer][pl.ds(pl.multiple_of(self.me * self.block_rows + (first + r), ROWS), ROWS), :] = new[0]
            self.m_out[k].at[layer][rows, :] = new[1]
            self.v_out[k].at[layer][rows, :] = new[2]

        by_rows(count, take)
        for s in (0, 1):
            self.gather_copy(p, s, 1, 1).start()

    def take_steps(self):
        self.loaded(0)
        self.states_loaded()
        for p in range(self.pieces):
            self.finish_sum(p)
            self.step(p)

    def spread(self, hop, spare=0):
        order = [self.live(s, hop + spare) for s in (0, 1)]
        for s in (0, 1):
            if hop == self.far - 1:
                order[s].sort(key=lambda p, s=s: -self.hops[p][s])
        for pair in zip(*order, strict=True):
            for s, p in enumerate(pair):
                self.gather_copy(p, s, hop - 1, 0).wait_recv()
                self.gather_copy(p, s, hop, 1).start()

    def last_hops(self, done):
        for p in range(self.pieces):
            for s in (0, 1):
                self.gather_copy(p, s, self.hops[p][s], 1, done).start()

    def gathered(self, spare):
        for hop in (self.far - 1, self.far):
            for p in range(self.pieces):
                for s in (0, 1):
                    if self.hops[p][s] == hop:
                        self.gather_copy(p, s, hop - spare, 0).wait_recv()

    def way_rows(self, spare):
        return sum((hops[0] - spare) * part[3] for hops, part in zip(self.hops, self.parts, strict=True))

    def all_sent(self, rows):
        for s in (0, 1):
            whole = self.inbox.at[pl.ds(0, rows)]
            pltpu.make_async_copy(whole, whole, self.send_sem.at[s]).wait()

    def greet(self):
        barrier = pltpu.get_barrier_semaphore()
        for neighbour in self.to:
            pl.semaphore_signal(barrier, inc=1, device_id={"dp": neighbour}, device_id_type=MESH)
        pl.semaphore_wait(barrier, 2)


def ahead():
    return lax.rem(lax.axis_index("rep"), 2) == 0


def behind():
    return lax.rem(lax.axis_index("rep"), 2) == 1


def early_kernel(n, shape, late_shape, *refs):
    refs = list(refs)
    take = lambda c: [refs.pop(0) for _ in range(c)]
    e, l = shape[0], late_shape[0]
    data, late_data = [take(e) for _ in range(4)], [take(l) for _ in range(4)]
    results, late_results = [take(e) for _ in range(3)], [take(l) for _ in range(3)]
    me = lax.axis_index("dp")
    ring = Ring(n, me, shape, EARLY_PIECES, *data, results, take(6), take(4))
    late = Ring(n, me, late_shape, LATE_PIECES, *late_data, late_results, take(6), take(4))

    ring.greet()
    pl.when(ahead())(late.first_terms)
    ring.first_terms()

    @pl.when(ahead())
    def _():
        late.load_terms()
        late.load_states()

    ring.load_terms()
    ring.load_states()

    @pl.when(ahead())
    def _():
        late.pass_on()
        late.take_steps()

    ring.pass_on()
    ring.take_steps()
    for hop in range(2, ring.far + 1):
        if hop < ring.far:
            pl.when(ahead())(functools.partial(late.spread, hop, 1))
        ring.spread(hop)
    ring.gathered(0)
    ring.all_sent(ring.way_rows(0) + ring.inbox_rows)

    @pl.when(ahead())
    def _():
        late.gathered(1)
        late.all_sent(late.way_rows(1) + late.inbox_rows)


def late_kernel(n, shape, *refs):
    refs = list(refs)
    take = lambda c: [refs.pop(0) for _ in range(c)]
    count = shape[0]
    data, done = [take(count) for _ in range(4)], take(count)
    results = [take(count) for _ in range(3)]
    ring = Ring(n, lax.axis_index("dp"), shape, LATE_PIECES, *data, results, take(6), take(4))
    ring.greet()

    @pl.when(ahead())
    def _():
        pl.delay(HOLD)
        ring.last_hops(done)

    @pl.when(behind())
    def _():
        ring.first_terms()
        ring.load_terms()
        ring.load_states()
        ring.pass_on()
        ring.take_steps()
        for hop in range(2, ring.far + 1):
            ring.spread(hop)

    ring.gathered(0)
    pl.when(ahead())(functools.partial(ring.all_sent, ring.way_rows(0) - ring.way_rows(1)))
    pl.when(behind())(functools.partial(ring.all_sent, ring.way_rows(0) + ring.inbox_rows))


def parted(n, shape, last):
    weights, _, rows, _ = shape
    parts, hops, *_ = Ring.cut(n, LATE_PIECES, shape)
    far, near = n // 2, (n - 1) // 2
    whole = [far] if last else range(1 - near, near)
    wanted = [(k, None, 0, rows, away) for k in range(weights) for away in whole]
    for p, (k, layer, first, count) in enumerate(parts):
        from_before = (hops[p][0] == far) != last
        wanted.append((k, layer, first, count, -near if from_before else near))
    return wanted


def put_early_kernel(n, e, shape, *refs):
    refs, sem = list(refs[:-1]), refs[-1]
    l = shape[0]
    count = 3 * (e + l)
    sources, results = refs[:count], refs[count:]
    early = [pltpu.make_async_copy(sources[i], results[i], sem.at[i]) for i in range(3 * e)]
    for copy in early:
        copy.start()

    @pl.when(ahead())
    def _():
        late = [pltpu.make_async_copy(sources[i], results[i], sem.at[i]) for i in range(3 * e + l, count)]
        late += block_copies(n, sources[3 * e : 3 * e + l], results[3 * e : 3 * e + l], parted(n, shape, False), sem, count)
        for copy in late:
            copy.start()
        for copy in late:
            copy.wait()

    for copy in early:
        copy.wait()


def block_copies(n, sources, results, wanted, sem, first_sem):
    me = lax.axis_index("dp")
    copies = []
    for k, layer, first, count, away in wanted:
        block_rows = sources[k].shape[1] // n
        rows = pl.ds(pl.multiple_of(lax.rem(me + (away + n), n) * block_rows + first, ROWS), count)
        at = (slice(None) if layer is None else layer, rows)
        copies.append(pltpu.make_async_copy(sources[k].at[at], results[k].at[at], sem.at[first_sem + len(copies)]))
    return copies


def put_late_kernel(n, shape, *refs):
    l = shape[0]
    sources, results, sem = refs[: 3 * l], refs[6 * l : 9 * l], refs[-1]

    @pl.when(ahead())
    def _():
        copies = block_copies(n, sources[:l], results[:l], parted(n, shape, True), sem, 3 * l)
        for copy in copies:
            copy.start()
        for copy in copies:
            copy.wait()

    @pl.when(behind())
    def _():
        copies = [pltpu.make_async_copy(sources[i], results[i], sem.at[i]) for i in range(3 * l)]
        for copy in copies:
            copy.start()
        for copy in copies:
            copy.wait()


def solution(mesh):
    n = mesh.shape["dp"]

    def step(*arrays):
        g, w, m, v = (arrays[i : i + 3] for i in (0, 3, 6, 9))
        early, late = slice(0, 2), slice(2, 3)
        e, l = len(g[early]), len(g[late])
        vmem = lambda several: [pltpu.VMEM(one.shape, one.dtype) for one in several]
        hbm = lambda several: [pltpu.HBM(one.shape, one.dtype) for one in several]
        early_shape, late_shape = (e, *m[early][0].shape), (l, *m[late][0].shape)
        early_results, late_results = (*w[early], *m[early], *v[early]), (*w[late], *m[late], *v[late])

        first = pl.pallas_call(
            functools.partial(early_kernel, n, early_shape, late_shape),
            out_shape=vmem((*early_results, *late_results)),
            in_specs=[HBM] * (4 * (e + l)),
            out_specs=[VMEM] * (3 * (e + l)),
            scratch_shapes=[*Ring.scratch(n, EARLY_PIECES, early_shape), *Ring.scratch(n, LATE_PIECES, late_shape)],
            compiler_params=pltpu.CompilerParams(collective_id=0, has_side_effects=True, vmem_limit_bytes=GRANT_EARLY),
        )(*g[early], *w[early], *m[early], *v[early], *g[late], *w[late], *m[late], *v[late])
        first = pl.pallas_call(
            functools.partial(put_early_kernel, n, e, late_shape),
            out_shape=hbm((*early_results, *late_results)),
            in_specs=[VMEM] * (3 * (e + l)),
            out_specs=[HBM] * (3 * (e + l)),
            scratch_shapes=[DMA((3 * (e + l) + len(parted(n, late_shape, False)),))],
            compiler_params=pltpu.CompilerParams(vmem_limit_bytes=1 << 20),
        )(*first)
        first, half = first[: 3 * e], first[3 * e :]
        second = pl.pallas_call(
            functools.partial(late_kernel, n, late_shape),
            out_shape=vmem(late_results),
            in_specs=[HBM] * (5 * l),
            out_specs=[VMEM] * (3 * l),
            scratch_shapes=Ring.scratch(n, LATE_PIECES, late_shape),
            compiler_params=pltpu.CompilerParams(collective_id=1, has_side_effects=True, vmem_limit_bytes=GRANT_LATE),
        )(*g[late], *w[late], *m[late], *v[late], *half[:l])
        second = pl.pallas_call(
            functools.partial(put_late_kernel, n, late_shape),
            out_shape=hbm(late_results),
            in_specs=[VMEM] * (3 * l) + [HBM] * (3 * l),
            out_specs=[HBM] * (3 * l),
            scratch_shapes=[DMA((3 * l + len(parted(n, late_shape, True)),))],
            input_output_aliases={3 * l + i: i for i in range(3 * l)},
            compiler_params=pltpu.CompilerParams(vmem_limit_bytes=1 << 20),
        )(*second, *half)
        return tuple(one for i in range(3) for one in (*first[i * e : (i + 1) * e], *second[i * l : (i + 1) * l]))

    all_of, cut = P(None, None, None), P(None, "dp", None)
    return jax.shard_map(
        step,
        mesh=mesh,
        in_specs=(P(("rep", "dp"), None, None, None),) * 3 + (all_of,) * 3 + (cut,) * 6,
        out_specs=(P("rep", None, None),) * 3 + (P("rep", "dp", None),) * 6,
        check_vma=False,
    )
```
